32 devices in a mesh: sweep: 2 (over y), expert: 4 (over z), dp: 4 (over x, core).
Axes of the slice: x: 2, y: 2, z: 4, core: 2. Of those that a mesh axis runs over, the one named last changes fastest.
Arguments:
- tokens: bfloat16 [4096, 1536], P(('sweep', 'expert', 'dp')), parts along dimension 0, may hold values from -6 to 6
- expert_ids: int32 [4096, 8], P(('sweep', 'expert', 'dp')), parts along dimension 0, may hold values from 0 to 63, all different within a row; in each aligned block of 128 rows (0 to 127, 128 to 255, ...) at most 20 rows name the same one
- gate_weights: float32 [4096, 8], P(('sweep', 'expert', 'dp')), parts along dimension 0, may hold values from 0.1 to 0.6
- expert_in: bfloat16 [128, 1536, 768], P(('sweep', 'expert'), 'dp'), parts along dimension 0, may hold values from -0.15625 to 0.15625
- expert_out: bfloat16 [128, 768, 1536], P(('sweep', 'expert'), None, 'dp'), parts along dimension 0, may hold values from -0.21875 to 0.21875
- shared_in: bfloat16 [3072, 768], P(('sweep', 'dp')), parts along dimension 0, may hold values from -0.15625 to 0.15625
- shared_out: bfloat16 [1536, 1536], P('sweep', 'dp'), parts along dimension 0, may hold values from -0.21875 to 0.21875
Outputs:
- block_out: bfloat16 [4096, 1536], P(('sweep', 'expert', 'dp')), parts along dimension 0
The draws below stay inside these ranges and needn't reach their ends.
There are 2 independent parts, one for each index of `sweep`. The reference program is written for one: setup_inputs(seed, part) draws one part's arguments, and reference() takes and returns one part's arrays. A program takes and returns all parts, laid end to end along the dimension named above; each array names one. Nothing has to cross between parts.
Inputs may be any that keep to these rules, and one draw needn't show every extreme that they name: `expert_ids`: each token names 8 different experts. In each aligned block of 128 tokens (the tokens of one device) no expert is named by more than 20 tokens; some blocks have an expert named by exactly 20.
All inputs are finite; a program needn't handle non-finite values.
Results may differ from the reference program's by a relative error of at most 0.0051.
Values may be sent and summed in bfloat16 or wider, within the bound.
No kernel may reach another device: no remote copies, remote signals or barrier semaphores. Data moves between devices by JAX's collectives and lax.ppermute only.
A program may use at most 192 MiB of HBM per device.

```python
import math
import jax
import jax.numpy as jnp
import numpy as np
from jax import lax

D = 1536
FF = 768
EXPERTS = 64
TOPK = 8
TOK_DEV = 128
CAP = 20
TOKENS = 2048


def levels(rng, shape, split, least, top_value):
    def one(position, parts):
        heights = jax.random.uniform(jax.random.fold_in(jax.random.fold_in(rng, 6), position), (parts,), jnp.float32, least / len(split), top_value / len(split))
        return jnp.repeat(jnp.exp(heights), shape[position] // parts).reshape((-1,) + (1,) * (len(shape) - position - 1))

    loudness = one(*split[0])
    for cut in split[1:]:
        loudness = loudness * one(*cut)
    return loudness


def assign_block(key, own, number, rows, amount, top, reach, slope):
    sequence = jax.random.permutation(key, amount)
    heavy_load, usual = load_shares(amount, rows * top, reach, slope, True), load_shares(amount, rows * top, reach, slope, False)
    places = jnp.arange(amount)

    def named(lengths, rotation):
        used = int((lengths > 0).sum())
        fixed = max(1, used // 4)
        moved = fixed + (places - fixed + rotation * (used - fixed)) % max(1, amount - fixed)
        return jnp.zeros((amount,), jnp.int32).at[sequence[jnp.where(places < fixed, places, moved)]].set(jnp.asarray(lengths, jnp.int32))

    lengths = jnp.where(number % 4 == 0, named(heavy_load, number // 4), named(usual, number - number // 4 - 1))
    mixed = jax.random.permutation(jax.random.fold_in(own, 3), amount)
    donor, taker = mixed[0:amount // 2 * 2:2], mixed[1:amount // 2 * 2:2]
    margin = jnp.minimum(lengths[donor] - 1, reach - lengths[taker]) // 2
    margin = jnp.where((donor == sequence[0]) | (taker == sequence[0]) | (lengths[taker] == 0), 0, jnp.maximum(margin, 0))
    moved = jax.random.randint(jax.random.fold_in(own, 4), (amount // 2,), 0, 1 << 20) % (margin + 1)
    lengths = lengths.at[donor].add(-moved).at[taker].add(moved)
    labels = jnp.searchsorted(jnp.cumsum(lengths), jnp.arange(rows * top), side="right").astype(jnp.int32)
    listing = labels.reshape(top, rows).T
    listing = listing[jax.random.permutation(jax.random.fold_in(own, 1), rows)]
    rotation = jax.random.randint(jax.random.fold_in(own, 2), (rows, 1), 0, top)
    return jnp.take_along_axis(listing, (jnp.arange(top)[None, :] + rotation) % top, axis=1)


def load_shares(amount, total, reach, lean, full):
    loads = [(1 << 20) // math.isqrt(grade ** lean) + 1 for grade in range(1, amount + 1)]
    largest = reach if full else min(reach, max(-(-total // amount), total * loads[0] // sum(loads)))
    least = 1 if total - largest >= amount - 1 else 0
    given, spare = [largest] + [least] * (amount - 1), total - largest - least * (amount - 1)
    while spare > 0:
        movable = [i for i in range(1, amount) if given[i] < largest] or [i for i in range(1, amount) if given[i] < reach]
        mass, budget = sum([loads[i] for i in movable]), spare
        for i in movable:
            extra = min(reach - given[i], max(1, budget * loads[i] // mass), spare)
            given[i] = given[i] + extra
            spare = spare - extra
    return np.array(given)


def scatter_about(own_key, dims, scale, limit, cuts=(), kind=jnp.bfloat16):
    level = levels(own_key, dims, cuts, -0.22, 0.18) if cuts else 1.0
    values = jax.random.normal(own_key, dims, jnp.float32) * scale * level
    return jnp.minimum(jnp.maximum(values, -limit), limit).astype(kind)


def setup_inputs(seed: int = 0, part: int = 0) -> dict:
    seeds = jax.random.split(jax.random.key(seed), 8)
    part_splits = jax.random.split(jax.random.fold_in(seeds[7], part), 8)
    tokens = scatter_about(part_splits[0], (TOKENS, D), 1.0, 6.0, ((0, 16),))
    expert_ids_keys = jax.random.split(jax.random.fold_in(part_splits[1], 1), TOKENS // TOK_DEV)
    expert_ids_turns = jax.random.permutation(jax.random.fold_in(part_splits[1], 3), TOKENS // TOK_DEV)
    expert_ids = jax.vmap(lambda own, number: assign_block(jax.random.fold_in(part_splits[1], 2), own, number, TOK_DEV, EXPERTS, TOPK, CAP, 2))(expert_ids_keys, expert_ids_turns).reshape((TOKENS, TOPK))
    gate_weights = jnp.clip(0.1 + 0.5 * jax.random.uniform(part_splits[2], (TOKENS, TOPK), jnp.float32) ** levels(part_splits[2], (TOKENS, TOPK), ((0, 16),), -0.2, 0.2), 0.1, 0.6)
    expert_in = scatter_about(part_splits[3], (EXPERTS, D, FF), D ** -0.5, 0.15625, ((0, 4), (1, 4)))
    expert_out = scatter_about(part_splits[4], (EXPERTS, FF, D), FF ** -0.5, 0.21875, ((0, 4), (2, 4)))
    shared_in = scatter_about(part_splits[5], (D, FF), D ** -0.5, 0.15625, ((0, 4),))
    shared_out = scatter_about(part_splits[6], (FF, D), FF ** -0.5, 0.21875, ((1, 4),))
    return dict(tokens=tokens, expert_ids=expert_ids, gate_weights=gate_weights, expert_in=expert_in, expert_out=expert_out, shared_in=shared_in, shared_out=shared_out)


def layer_norm(tokens):
    values = tokens.astype(jnp.float32)
    center = values - lax.optimization_barrier(jnp.mean(values, axis=-1, keepdims=True))
    spread = lax.optimization_barrier(jnp.mean(center * center, axis=-1, keepdims=True))
    return (center * lax.rsqrt(spread + 1e-06)).astype(jnp.bfloat16)

def reference(tokens, expert_ids, gate_weights, expert_in, expert_out, shared_in, shared_out):
    normed = layer_norm(tokens)
    token_count = tokens.shape[0]
    model_width = tokens.shape[1]
    expert_count = expert_in.shape[0]
    place_count = token_count // TOK_DEV * CAP
    expert_iota = jnp.arange(expert_count, dtype=jnp.int32)
    matches = (expert_ids[:, :, None] == expert_iota[None, None, :]).astype(jnp.int32)
    per_token = lax.optimization_barrier(jnp.sum(matches, axis=1, dtype=jnp.int32))
    earlier = jnp.cumsum(per_token, axis=0, dtype=jnp.int32) - per_token
    slot_of = jnp.take_along_axis(earlier, expert_ids, axis=1).astype(jnp.int32)
    anchors = jnp.broadcast_to(jnp.arange(token_count, dtype=jnp.int32)[:, None], expert_ids.shape)
    slot_table = jnp.full((expert_count, place_count), token_count, jnp.int32)
    slot_table = slot_table.at[expert_ids, slot_of].set(anchors)
    gate_table = jnp.zeros((expert_count, place_count), jnp.float32)
    gate_table = gate_table.at[expert_ids, slot_of].set(gate_weights.astype(jnp.float32))
    padded = jnp.concatenate([normed, jnp.zeros((1, model_width), jnp.bfloat16)], axis=0)

    def expert_step(summed, inputs):
        row_index, gate_rows, weight_in, weight_out = inputs
        gathered = padded[row_index]
        hidden = jax.nn.gelu(jnp.dot(gathered, weight_in, preferred_element_type=jnp.float32)).astype(jnp.bfloat16)
        result = jnp.dot(hidden, weight_out, preferred_element_type=jnp.float32).astype(jnp.bfloat16)
        summed = summed.at[row_index].add(result.astype(jnp.float32) * gate_rows[:, None])
        return (summed, None)
    start_sum = jnp.zeros((token_count + 1, model_width), jnp.float32)
    summed, _ = lax.scan(expert_step, start_sum, (slot_table, gate_table, expert_in, expert_out))
    routed = summed[:token_count]
    shared_hidden = jax.nn.gelu(jnp.dot(normed, shared_in, preferred_element_type=jnp.float32)).astype(jnp.bfloat16)
    shared_result = jnp.dot(shared_hidden, shared_out, preferred_element_type=jnp.float32)
    return (tokens.astype(jnp.float32) + shared_result + routed).astype(jnp.bfloat16)
```

```python
import functools

import jax
import jax.numpy as jnp
from jax import lax
from jax.experimental import pallas as pl
from jax.experimental.pallas import tpu as pltpu
from jax.sharding import PartitionSpec as P

CAP = 20
F32 = jnp.float32
BF16 = jnp.bfloat16
META = 16


def layer_norm(tokens):
    values = tokens.astype(F32)
    center = values - jnp.mean(values, axis=-1, keepdims=True)
    spread = jnp.mean(center * center, axis=-1, keepdims=True)
    return (center * lax.rsqrt(spread + 1e-06)).astype(BF16)


def copy_slots(expert_ids, expert_count):
    expert_iota = jnp.arange(expert_count, dtype=jnp.int32)
    matches = (expert_ids[..., None] == expert_iota).astype(jnp.int32)
    per_token = jnp.sum(matches, axis=-2, dtype=jnp.int32)
    earlier = jnp.cumsum(per_token, axis=-2, dtype=jnp.int32) - per_token
    return jnp.sum(matches * earlier[..., None, :], axis=-1, dtype=jnp.int32)


def run_experts(shard_piece, weight_in, weight_out):
    pre_act = jnp.einsum("gesd,edf->gesf", shard_piece, weight_in, preferred_element_type=F32)
    hidden = jax.nn.gelu(pre_act).astype(BF16)
    return jnp.einsum("gesf,efd->gesd", hidden, weight_out, preferred_element_type=F32).astype(BF16)


def gathered_weights(tokens, expert_ids, gate_weights, expert_in, expert_out, shared_in, shared_out):
    row_count, model_width = tokens.shape
    pick_count = expert_ids.shape[1]
    local_count = expert_in.shape[0]
    group_count = lax.axis_size("expert")
    expert_total = local_count * group_count
    normed = layer_norm(tokens)
    full_in = lax.all_gather(expert_in, "dp", axis=1, tiled=True)
    full_out = lax.all_gather(expert_out, "dp", axis=2, tiled=True)
    slot_of = copy_slots(expert_ids, expert_total)
    positions = (expert_ids * CAP + slot_of).reshape(-1)
    copies = jnp.repeat(normed, pick_count, axis=0)
    outgoing = jnp.zeros((expert_total * CAP, model_width), BF16).at[positions].set(copies)
    outgoing = outgoing.reshape(group_count, local_count, CAP, model_width)
    received = lax.all_to_all(outgoing, "expert", split_axis=0, concat_axis=0, tiled=True)
    returned = lax.all_to_all(
        run_experts(received, full_in, full_out), "expert", split_axis=0, concat_axis=0, tiled=True
    )
    results = returned.reshape(expert_total * CAP, model_width)[positions].reshape(
        row_count, pick_count, model_width
    )
    routed = jnp.sum(results.astype(F32) * gate_weights[:, :, None], axis=1)
    shared_pre = jnp.dot(
        normed, lax.all_gather(shared_in, "dp", axis=0, tiled=True), preferred_element_type=F32
    )
    shared_hidden = jax.nn.gelu(shared_pre).astype(BF16)
    shared_result = jnp.dot(
        shared_hidden,
        lax.all_gather(shared_out, "dp", axis=1, tiled=True),
        preferred_element_type=F32,
    )
    return (tokens.astype(F32) + shared_result + routed).astype(BF16)


def dot(a, b):
    return jnp.dot(a, b, preferred_element_type=F32)


def swap(value, axis, mask):
    size = lax.axis_size(axis)
    return lax.ppermute(value, axis, [(i, i ^ mask) for i in range(size)])


def cost(flops, moved):
    return pl.CostEstimate(flops=int(flops), bytes_accessed=int(moved), transcendentals=0)


def norm_kernel(place, tokens, ids, gates, mine, theirs):
    rows, width = tokens.shape
    half = width // 2
    values = tokens[...].astype(F32)
    center = values - jnp.mean(values, axis=-1, keepdims=True)
    spread = jnp.mean(center * center, axis=-1, keepdims=True)
    normed = (center * lax.rsqrt(spread + 1e-06)).astype(BF16)
    low = place[1] == 0
    mine[0:rows, :] = jnp.where(low, normed[:, :half], normed[:, half:])
    theirs[0:rows, :] = jnp.where(low, normed[:, half:], normed[:, :half])
    gate = gates[...]
    high = gate.astype(BF16).astype(F32)
    rest = gate - high
    picks = ids.shape[0]
    spare = jnp.zeros((picks, half - 3 * rows), F32)
    table = jnp.concatenate([ids[...].astype(F32), high, rest, spare], axis=1)
    table = jnp.concatenate([table, jnp.zeros((META - picks, half), F32)], axis=0).astype(BF16)
    mine[rows : rows + META, :] = table
    theirs[rows : rows + META, :] = table


def selection(codes, rows):
    count, tokens = codes.shape
    wanted = lax.broadcasted_iota(jnp.int32, (rows, tokens), 0).astype(F32)
    return [(wanted == codes[e : e + 1, :]).astype(F32) for e in range(count)]


def first_kernel(units, picks, place, *refs):
    feeds, (own, other, part, code, gate, packed) = refs[:units], refs[units:]
    local, rows, half = packed.shape
    slots = rows // (2 * units)
    tokens = feeds[0].shape[0] // 2 - META
    step = pl.program_id(0)

    @pl.when(step == 0)
    def _():
        lead = place[2]
        before = (
            lax.broadcasted_iota(jnp.int32, (tokens, tokens), 0)
            < lax.broadcasted_iota(jnp.int32, (tokens, tokens), 1)
        ).astype(F32).astype(BF16)
        expert = (lax.broadcasted_iota(jnp.int32, (local, tokens), 0) + lead).astype(F32)
        for u in range(units):
            for b in range(2):
                at = 2 * tokens + b * META
                table = feeds[u][at : at + META, 0 : 3 * tokens].astype(F32)
                named = jnp.zeros((local, tokens), F32)
                weight = jnp.zeros((local, tokens), F32)
                for k in range(picks):
                    same = table[k : k + 1, 0:tokens] == expert
                    value = table[k : k + 1, tokens : 2 * tokens] + table[k : k + 1, 2 * tokens :]
                    named = jnp.where(same, 1.0, named)
                    weight = jnp.where(same, value, weight)
                rank = dot(named.astype(BF16), before)
                turn = place[1] if b == 0 else 1 - place[1]
                base = ((2 * u + turn) * slots).astype(F32)
                column = (2 * u + b) * tokens
                code[:, column : column + tokens] = jnp.where(named > 0, rank + base, -1.0)
                gate[:, column : column + tokens] = weight
        pick = jnp.concatenate(selection(code[...], rows), axis=0).astype(BF16)
        wide = half // 3 if half % 384 == 0 else half
        for n in range(half // wide):
            columns = slice(n * wide, (n + 1) * wide)
            chosen = sum(
                dot(pick[:, 2 * u * tokens : 2 * (u + 1) * tokens], feeds[u][0 : 2 * tokens, columns])
                for u in range(units)
            )
            for e in range(local):
                packed[e, :, columns] = chosen[e * rows : (e + 1) * rows].astype(BF16)

    quarter = half // 2
    here = pl.multiple_of(place[0] * quarter, quarter)
    there = pl.multiple_of((1 - place[0]) * quarter, quarter)
    total = dot(packed[step, :, pl.ds(here, quarter)], own[0])
    total += dot(packed[step, :, pl.ds(there, quarter)], other[0])
    part[0] = total.astype(BF16)


def second_kernel(units, keep, send, place, *refs):
    code, gate, near, far, own, other = refs[:6]
    outs, total = refs[6:-1], refs[-1]
    local = code.shape[0]
    rows, hidden_width = near.shape[1:]
    half = total.shape[1]
    step = pl.program_id(0)
    wanted = lax.broadcasted_iota(jnp.int32, (rows, code.shape[1]), 0).astype(F32)
    same = wanted == code[pl.ds(step, 1), :]
    scale = jnp.sum(jnp.where(same, gate[pl.ds(step, 1), :], 0.0), axis=1, keepdims=True)
    hidden = jax.nn.gelu(near[0].astype(F32) + far[0].astype(F32)).astype(BF16)
    quarter = half // 2
    here = pl.multiple_of(place[0] * quarter, quarter)
    there = pl.multiple_of((1 - place[0]) * quarter, quarter)
    at = pl.ds(pl.multiple_of(step * rows, rows), rows)
    total[at, pl.ds(here, quarter)] = dot(hidden, own[0]) * scale
    total[at, pl.ds(there, quarter)] = dot(hidden, other[0]) * scale

    @pl.when(step == local - 1)
    def _():
        pick = jnp.concatenate(selection(code[...], rows), axis=0).astype(BF16)
        wide = half // 3 if half % 384 == 0 else half
        count = code.shape[1] // units
        for n in range(half // wide):
            columns = slice(n * wide, (n + 1) * wide)
            summed = lax.dot_general(
                pick,
                total[:, columns].astype(BF16),
                (((0,), (0,)), ((), ())),
                preferred_element_type=F32,
            )
            slot = 0
            if keep:
                outs[slot][:, columns] = summed[0:count]
                slot += 1
            if send:
                outs[slot][:, columns] = summed[(units - 1) * count :].astype(BF16)


def first_stage(feeds, place, own, other, picks):
    units = len(feeds)
    local, quarter, hidden = other.shape
    half = 2 * quarter
    tokens = feeds[0].shape[0] // 2 - META
    rows = 2 * units * CAP
    whole = lambda e, s: (0, 0)
    return pl.pallas_call(
        functools.partial(first_kernel, units, picks),
        grid_spec=pltpu.PrefetchScalarGridSpec(
            num_scalar_prefetch=1,
            grid=(local,),
            in_specs=[pl.BlockSpec(f.shape, whole) for f in feeds]
            + [
                pl.BlockSpec((1, quarter, hidden), lambda e, s: (s[0] * local + e, 0, 0)),
                pl.BlockSpec((1, quarter, hidden), lambda e, s: (e, 0, 0)),
            ],
            out_specs=[
                pl.BlockSpec((1, rows, hidden), lambda e, s: (e, 0, 0)),
                pl.BlockSpec((local, 2 * units * tokens), whole),
                pl.BlockSpec((local, 2 * units * tokens), whole),
            ],
            scratch_shapes=[pltpu.VMEM((local, rows, half), BF16)],
        ),
        out_shape=[
            jax.ShapeDtypeStruct((local, rows, hidden), BF16),
            jax.ShapeDtypeStruct((local, 2 * units * tokens), F32),
            jax.ShapeDtypeStruct((local, 2 * units * tokens), F32),
        ],
        cost_estimate=cost(2 * local * rows * half * hidden, 2 * local * half * hidden),
        name=f"first_{units}",
    )(place, *feeds, own, other)


def second_stage(units, code, gate, near, far, place, own, other, keep, send):
    local, hidden, quarter = other.shape
    half = 2 * quarter
    rows = near.shape[1]
    count = code.shape[1] // units
    whole = lambda e, s: (0, 0)
    shapes = []
    if keep:
        shapes.append(jax.ShapeDtypeStruct((count, half), F32))
    if send:
        shapes.append(jax.ShapeDtypeStruct((count, half), BF16))
    return pl.pallas_call(
        functools.partial(second_kernel, units, keep, send),
        grid_spec=pltpu.PrefetchScalarGridSpec(
            num_scalar_prefetch=1,
            grid=(local,),
            in_specs=[
                pl.BlockSpec(code.shape, whole),
                pl.BlockSpec(gate.shape, whole),
                pl.BlockSpec((1, rows, hidden), lambda e, s: (e, 0, 0)),
                pl.BlockSpec((1, rows, hidden), lambda e, s: (e, 0, 0)),
                pl.BlockSpec((1, hidden, quarter), lambda e, s: (s[0] * local + e, 0, 0)),
                pl.BlockSpec((1, hidden, quarter), lambda e, s: (e, 0, 0)),
            ],
            out_specs=[pl.BlockSpec(s.shape, whole) for s in shapes],
            scratch_shapes=[pltpu.VMEM((local * rows, half), F32)],
        ),
        out_shape=shapes,
        cost_estimate=cost(2 * local * rows * half * hidden, 2 * local * half * hidden),
        name=f"second_{units}",
    )(place, code, gate, near, far, own, other)


def shared_first_kernel(place, feed, own, other, part):
    quarter = own.shape[0]
    rows = part.shape[0] // 2
    here = pl.multiple_of(place[0] * quarter, quarter)
    there = pl.multiple_of((1 - place[0]) * quarter, quarter)
    total = dot(feed[0 : 2 * rows, pl.ds(here, quarter)], own[...])
    total += dot(feed[0 : 2 * rows, pl.ds(there, quarter)], other[...])
    for b in range(2):
        turn = place[1] if b == 0 else 1 - place[1]
        at = pl.ds(pl.multiple_of(turn * rows, rows), rows)
        part[at, :] = total[b * rows : (b + 1) * rows].astype(BF16)


def shared_second_kernel(place, near, far, own, other, out):
    quarter = own.shape[1]
    rows = near.shape[0] // 2
    here = pl.multiple_of(place[0] * quarter, quarter)
    there = pl.multiple_of((1 - place[0]) * quarter, quarter)
    hidden = jax.nn.gelu(near[...].astype(F32) + far[...].astype(F32)).astype(BF16)
    left, right = dot(hidden, own[...]), dot(hidden, other[...])
    for b in range(2):
        turn = place[1] if b == 0 else 1 - place[1]
        at = pl.ds(pl.multiple_of(turn * rows, rows), rows)
        out[at, pl.ds(here, quarter)] = left[b * rows : (b + 1) * rows]
        out[at, pl.ds(there, quarter)] = right[b * rows : (b + 1) * rows]


SMEM = pl.BlockSpec(memory_space=pltpu.SMEM)
VMEM = pl.BlockSpec(memory_space=pltpu.VMEM)


def exchanged_partials(tokens, expert_ids, gate_weights, expert_in, expert_out, shared_in, shared_out):
    rows, width = tokens.shape
    half = width // 2
    picks = expert_ids.shape[1]
    group = expert_in.shape[0]
    local = group // 2
    hidden = expert_in.shape[2]
    groups = lax.axis_size("expert")
    spot = lax.axis_index("dp")
    side, core = spot // 2, spot % 2
    lead = lax.axis_index("expert") * group + core * local
    place = jnp.stack([core, side, lead]).astype(jnp.int32)

    give_in = lax.dynamic_slice_in_dim(expert_in, (1 - core) * local, local, 0)
    other_in = swap(give_in, "dp", 1)
    mine, theirs = pl.pallas_call(
        norm_kernel,
        in_specs=[SMEM, VMEM, VMEM, VMEM],
        out_specs=[VMEM, VMEM],
        out_shape=[jax.ShapeDtypeStruct((rows + META, half), BF16)] * 2,
        cost_estimate=cost(20 * rows * width, 4 * rows * width),
        name="norm",
    )(place, tokens, expert_ids.T, gate_weights.T)
    peer = swap(theirs, "dp", 2)
    other_shared_in = swap(shared_in, "dp", 1)
    give_out = lax.dynamic_slice_in_dim(expert_out, (1 - core) * local, local, 0)
    other_out = swap(give_out, "dp", 1)
    other_shared_out = swap(shared_out, "dp", 1)

    unit = jnp.concatenate([mine[:rows], peer[:rows], mine[rows:], peer[rows:]], axis=0)
    away = [(g, swap(unit, "expert", g)) for g in range(1, groups)]
    beside = swap(unit, "dp", 1)

    chunks = [([unit], True, False)]
    for _, got in away:
        chunks.append(([got, swap(got, "dp", 1)], True, True))
    chunks.append(([beside], False, True))

    firsts = []
    for feeds, _, _ in chunks:
        part, code, gate = first_stage(feeds, place, expert_in, other_in, picks)
        firsts.append((part, code, gate, swap(part, "dp", 2)))
    shared_part = pl.pallas_call(
        shared_first_kernel,
        in_specs=[SMEM, VMEM, VMEM, VMEM],
        out_specs=VMEM,
        out_shape=jax.ShapeDtypeStruct((2 * rows, hidden), BF16),
        cost_estimate=cost(4 * rows * half * hidden, 2 * half * hidden),
        name="shared_first",
    )(place, unit, shared_in, other_shared_in)
    shared_far = swap(shared_part, "dp", 2)

    total = None
    for i, ((feeds, keep, send), (part, code, gate, far)) in enumerate(zip(chunks, firsts)):
        outs = second_stage(
            len(feeds), code, gate, part, far, place, expert_out, other_out, keep, send
        )
        if keep and not send:
            piece = outs[0]
        elif keep:
            joined = (outs[0] + swap(outs[1], "dp", 1).astype(F32)).astype(BF16)
            piece = swap(joined, "expert", away[i - 1][0]).astype(F32)
        else:
            piece = swap(outs[0], "dp", 1).astype(F32)
        total = piece if total is None else total + piece
    shared = pl.pallas_call(
        shared_second_kernel,
        in_specs=[SMEM, VMEM, VMEM, VMEM, VMEM],
        out_specs=VMEM,
        out_shape=jax.ShapeDtypeStruct((2 * rows, half), F32),
        cost_estimate=cost(4 * rows * half * hidden, 2 * half * hidden),
        name="shared_second",
    )(place, shared_part, shared_far, shared_out, other_shared_out)
    total = total + shared
    cross = swap(total[rows:].astype(BF16), "dp", 2).astype(F32)
    kept = total[:rows]
    low = side == 0
    added = jnp.concatenate([jnp.where(low, kept, cross), jnp.where(low, cross, kept)], axis=1)
    return (tokens.astype(F32) + added).astype(BF16)


def per_device(*args):
    tokens, expert_ids, expert_in = args[0], args[1], args[3]
    groups = lax.axis_size("expert")
    fits = (
        lax.axis_size("dp") == 4
        and expert_in.shape[0] % 16 == 0
        and groups & (groups - 1) == 0
        and groups <= 8
        and tokens.shape[0] % 128 == 0
        and tokens.shape[1] % 512 == 0
        and tokens.shape[1] // 2 >= 3 * tokens.shape[0]
        and expert_ids.shape[1] <= 8
        and expert_in.shape[2] % 128 == 0
    )
    return exchanged_partials(*args) if fits else gathered_weights(*args)


def solution(mesh):
    placed = (
        P(("sweep", "expert", "dp"), None),
        P(("sweep", "expert", "dp"), None),
        P(("sweep", "expert", "dp"), None),
        P(("sweep", "expert"), "dp", None),
        P(("sweep", "expert"), None, "dp"),
        P(("sweep", "dp"), None),
        P("sweep", "dp"),
    )
    return jax.shard_map(
        per_device,
        mesh=mesh,
        in_specs=placed,
        out_specs=P(("sweep", "expert", "dp"), None),
        check_vma=False,
    )
```

```python
import functools

import jax
import jax.numpy as jnp
from jax import lax
from jax.experimental import pallas as pl
from jax.experimental.pallas import tpu as pltpu
from jax.sharding import PartitionSpec as P


CAP = 20
F32 = jnp.float32
BF16 = jnp.bfloat16
KERNEL_FLOPS = 10_000_000
META = 16


def layer_norm(tokens):
    values = tokens.astype(F32)
    center = values - jnp.mean(values, axis=-1, keepdims=True)
    spread = jnp.mean(center * center, axis=-1, keepdims=True)
    return (center * lax.rsqrt(spread + 1e-06)).astype(BF16)


def copy_slots(expert_ids, expert_count):
    expert_iota = jnp.arange(expert_count, dtype=jnp.int32)
    matches = (expert_ids[..., None] == expert_iota).astype(jnp.int32)
    per_token = jnp.sum(matches, axis=-2, dtype=jnp.int32)
    earlier = jnp.cumsum(per_token, axis=-2, dtype=jnp.int32) - per_token
    return jnp.sum(matches * earlier[..., None, :], axis=-1, dtype=jnp.int32)


def run_experts(shard_piece, weight_in, weight_out):
    pre_act = jnp.einsum("gesd,edf->gesf", shard_piece, weight_in, preferred_element_type=F32)
    hidden = jax.nn.gelu(pre_act).astype(BF16)
    return jnp.einsum("gesf,efd->gesd", hidden, weight_out, preferred_element_type=F32).astype(BF16)


def gathered_weights(tokens, expert_ids, gate_weights, expert_in, expert_out, shared_in, shared_out):
    row_count, model_width = tokens.shape
    pick_count = expert_ids.shape[1]
    local_count = expert_in.shape[0]
    group_count = lax.axis_size("expert")
    expert_total = local_count * group_count
    normed = layer_norm(tokens)
    full_in = lax.all_gather(expert_in, "dp", axis=1, tiled=True)
    full_out = lax.all_gather(expert_out, "dp", axis=2, tiled=True)
    slot_of = copy_slots(expert_ids, expert_total)
    positions = (expert_ids * CAP + slot_of).reshape(-1)
    copies = jnp.repeat(normed, pick_count, axis=0)
    outgoing = jnp.zeros((expert_total * CAP, model_width), BF16).at[positions].set(copies)
    outgoing = outgoing.reshape(group_count, local_count, CAP, model_width)
    received = lax.all_to_all(outgoing, "expert", split_axis=0, concat_axis=0, tiled=True)
    returned = lax.all_to_all(
        run_experts(received, full_in, full_out), "expert", split_axis=0, concat_axis=0, tiled=True
    )
    results = returned.reshape(expert_total * CAP, model_width)[positions].reshape(
        row_count, pick_count, model_width
    )
    routed = jnp.sum(results.astype(F32) * gate_weights[:, :, None], axis=1)
    shared_pre = jnp.dot(
        normed, lax.all_gather(shared_in, "dp", axis=0, tiled=True), preferred_element_type=F32
    )
    shared_hidden = jax.nn.gelu(shared_pre).astype(BF16)
    shared_result = jnp.dot(
        shared_hidden,
        lax.all_gather(shared_out, "dp", axis=1, tiled=True),
        preferred_element_type=F32,
    )
    return (tokens.astype(F32) + shared_result + routed).astype(BF16)


def dot(a, b):
    return jnp.dot(a, b, preferred_element_type=F32)


def swap(value, axis, mask):
    size = lax.axis_size(axis)
    return lax.ppermute(value, axis, [(i, i ^ mask) for i in range(size)])


def cost(flops, moved):
    return pl.CostEstimate(flops=int(flops), bytes_accessed=int(moved), transcendentals=0)


def norm_kernel(place, tokens, ids, gates, source, mine, theirs, given, held, came, left):
    local = held.shape[0]
    base = (1 - place[0]) * local

    def fetch(e):
        return pltpu.make_async_copy(source.at[base + e], held.at[e], came.at[e])

    def put(e):
        return pltpu.make_async_copy(held.at[e], given.at[e], left.at[e])

    for e in range(local):
        fetch(e).start()
    rows, width = tokens.shape
    half = width // 2
    values = tokens[...].astype(F32)
    center = values - jnp.mean(values, axis=-1, keepdims=True)
    spread = jnp.mean(center * center, axis=-1, keepdims=True)
    normed = (center * lax.rsqrt(spread + 1e-06)).astype(BF16)
    low = place[1] == 0
    mine[0:rows, :] = jnp.where(low, normed[:, :half], normed[:, half:])
    theirs[0:rows, :] = jnp.where(low, normed[:, half:], normed[:, :half])
    gate = gates[...]
    high = gate.astype(BF16).astype(F32)
    rest = gate - high
    picks = ids.shape[0]
    spare = jnp.zeros((picks, half - 3 * rows), F32)
    table = jnp.concatenate([ids[...].astype(F32), high, rest, spare], axis=1)
    table = jnp.concatenate([table, jnp.zeros((META - picks, half), F32)], axis=0).astype(BF16)
    mine[rows : rows + META, :] = table
    theirs[rows : rows + META, :] = table
    for e in range(local):
        fetch(e).wait()
        put(e).start()
    for e in range(local):
        put(e).wait()


def give_kernel(place, source, after, given, held, came, left):
    local = held.shape[0]
    base = (1 - place[0]) * local

    def fetch(e):
        return pltpu.make_async_copy(source.at[base + e], held.at[e], came.at[e])

    def put(e):
        return pltpu.make_async_copy(held.at[e], given.at[e], left.at[e])

    for e in range(local):
        fetch(e).start()
    for e in range(local):
        fetch(e).wait()
        put(e).start()
    for e in range(local):
        put(e).wait()


def selection(codes, rows):
    count, tokens = codes.shape
    wanted = lax.broadcasted_iota(jnp.int32, (rows, tokens), 0).astype(F32)
    return [(wanted == codes[e : e + 1, :]).astype(F32) for e in range(count)]


def weight_copies(place, own, other, held_own, held_other, came):
    local = held_own.shape[0]

    def copies(e):
        return (
            pltpu.make_async_copy(own.at[place[0] * local + e], held_own.at[e], came.at[0, e]),
            pltpu.make_async_copy(other.at[e], held_other.at[e], came.at[1, e]),
        )

    return copies


def first_kernel(units, picks, place, *refs):
    feeds, refs = refs[:units], refs[units:]
    own, other, _, part, code, gate, packed, held_own, held_other, made, came, left = refs
    local, rows, half = packed.shape
    slots = rows // (2 * units)
    tokens = feeds[0].shape[0] // 2 - META
    copies = weight_copies(place, own, other, held_own, held_other, came)
    for e in range(local):
        for c in copies(e):
            c.start()

    before = (
        lax.broadcasted_iota(jnp.int32, (tokens, tokens), 0)
        < lax.broadcasted_iota(jnp.int32, (tokens, tokens), 1)
    ).astype(F32).astype(BF16)
    expert = (lax.broadcasted_iota(jnp.int32, (local, tokens), 0) + place[2]).astype(F32)
    for u in range(units):
        for b in range(2):
            at = 2 * tokens + b * META
            table = feeds[u][at : at + META, 0 : 3 * tokens].astype(F32)
            named = jnp.zeros((local, tokens), F32)
            weight = jnp.zeros((local, tokens), F32)
            for k in range(picks):
                same = table[k : k + 1, 0:tokens] == expert
                value = table[k : k + 1, tokens : 2 * tokens] + table[k : k + 1, 2 * tokens :]
                named = jnp.where(same, 1.0, named)
                weight = jnp.where(same, value, weight)
            rank = dot(named.astype(BF16), before)
            turn = place[1] if b == 0 else 1 - place[1]
            base = ((2 * u + turn) * slots).astype(F32)
            column = (2 * u + b) * tokens
            code[:, column : column + tokens] = jnp.where(named > 0, rank + base, -1.0)
            gate[:, column : column + tokens] = weight
    pick = jnp.concatenate(selection(code[...], rows), axis=0).astype(BF16)
    wide = half // 3 if half % 384 == 0 else half
    for n in range(half // wide):
        columns = slice(n * wide, (n + 1) * wide)
        chosen = sum(
            dot(pick[:, 2 * u * tokens : 2 * (u + 1) * tokens], feeds[u][0 : 2 * tokens, columns])
            for u in range(units)
        )
        for e in range(local):
            packed[e, :, columns] = chosen[e * rows : (e + 1) * rows].astype(BF16)

    quarter = half // 2
    here = pl.multiple_of(place[0] * quarter, quarter)
    there = pl.multiple_of((1 - place[0]) * quarter, quarter)

    def put(e):
        return pltpu.make_async_copy(made.at[e], part.at[e], left.at[e])

    @pl.loop(0, local // 2)
    def _(pair):
        for e in (2 * pair, 2 * pair + 1):
            for c in copies(e):
                c.wait()
            total = dot(packed[e, :, pl.ds(here, quarter)], held_own[e])
            total += dot(packed[e, :, pl.ds(there, quarter)], held_other[e])
            made[e] = total.astype(BF16)
        for e in (2 * pair, 2 * pair + 1):
            put(e).start()

    @pl.loop(0, local)
    def _(e):
        put(e).wait()


def second_kernel(units, keep, send, place, *refs):
    code, gate, near, far, own, other, _ = refs[:7]
    outs, (total, held_own, held_other, came) = refs[7:-4], refs[-4:]
    local = code.shape[0]
    rows = near.shape[1]
    half = total.shape[1]
    copies = weight_copies(place, own, other, held_own, held_other, came)
    for e in range(local):
        for c in copies(e):
            c.start()
    quarter = half // 2
    here = pl.multiple_of(place[0] * quarter, quarter)
    there = pl.multiple_of((1 - place[0]) * quarter, quarter)
    wanted = lax.broadcasted_iota(jnp.int32, (rows, code.shape[1]), 0).astype(F32)

    @pl.loop(0, local // 2)
    def _(pair):
        for e in (2 * pair, 2 * pair + 1):
            same = wanted == code[pl.ds(e, 1), :]
            scale = jnp.sum(jnp.where(same, gate[pl.ds(e, 1), :], 0.0), axis=1, keepdims=True)
            hidden = jax.nn.gelu(near[e].astype(F32) + far[e].astype(F32)).astype(BF16)
            for c in copies(e):
                c.wait()
            at = pl.ds(pl.multiple_of(e * rows, rows), rows)
            total[at, pl.ds(here, quarter)] = dot(hidden, held_own[e]) * scale
            total[at, pl.ds(there, quarter)] = dot(hidden, held_other[e]) * scale

    pick = jnp.concatenate(selection(code[...], rows), axis=0).astype(BF16)
    wide = half // 3 if half % 384 == 0 else half
    count = code.shape[1] // units
    for n in range(half // wide):
        columns = slice(n * wide, (n + 1) * wide)
        summed = lax.dot_general(
            pick,
            total[:, columns].astype(BF16),
            (((0,), (0,)), ((), ())),
            preferred_element_type=F32,
        )
        slot = 0
        if keep:
            outs[slot][:, columns] = summed[0:count]
            slot += 1
        if send:
            outs[slot][:, columns] = summed[(units - 1) * count :].astype(BF16)


SMEM = pl.BlockSpec(memory_space=pltpu.SMEM)
VMEM = pl.BlockSpec(memory_space=pltpu.VMEM)
ANY = pl.BlockSpec(memory_space=pl.ANY)
HBM = pl.BlockSpec(memory_space=pltpu.HBM)
GRANT = 55 << 20


def give_scratch(local, shape):
    return [
        pltpu.VMEM((local, *shape), BF16),
        pltpu.SemaphoreType.DMA((local,)),
        pltpu.SemaphoreType.DMA((local,)),
    ]


def first_stage(feeds, place, own, other, after, picks):
    units = len(feeds)
    local, quarter, hidden = other.shape
    half = 2 * quarter
    tokens = feeds[0].shape[0] // 2 - META
    rows = 2 * units * CAP
    table = jax.ShapeDtypeStruct((local, 2 * units * tokens), F32)
    return pl.pallas_call(
        functools.partial(first_kernel, units, picks),
        in_specs=[SMEM] + [VMEM] * units + [HBM, HBM, ANY],
        out_specs=[ANY, VMEM, VMEM],
        scratch_shapes=[
            pltpu.VMEM((local, rows, half), BF16),
            pltpu.VMEM((local, quarter, hidden), BF16),
            pltpu.VMEM((local, quarter, hidden), BF16),
            pltpu.VMEM((local, rows, hidden), BF16),
            pltpu.SemaphoreType.DMA((2, local)),
            pltpu.SemaphoreType.DMA((local,)),
        ],
        out_shape=[jax.ShapeDtypeStruct((local, rows, hidden), BF16), table, table],
        compiler_params=pltpu.CompilerParams(vmem_limit_bytes=GRANT),
        cost_estimate=cost(KERNEL_FLOPS, 2 * local * half * hidden),
    )(place, *feeds, own, other, after)


def second_stage(units, code, gate, near, far, place, own, other, after, keep, send):
    local, hidden, quarter = other.shape
    half = 2 * quarter
    rows = near.shape[1]
    count = code.shape[1] // units
    shapes = []
    if keep:
        shapes.append(jax.ShapeDtypeStruct((count, half), F32))
    if send:
        shapes.append(jax.ShapeDtypeStruct((count, half), BF16))
    return pl.pallas_call(
        functools.partial(second_kernel, units, keep, send),
        in_specs=[SMEM] + [VMEM] * 4 + [HBM, HBM, ANY],
        out_specs=[VMEM] * len(shapes),
        scratch_shapes=[
            pltpu.VMEM((local * rows, half), F32),
            pltpu.VMEM((local, hidden, quarter), BF16),
            pltpu.VMEM((local, hidden, quarter), BF16),
            pltpu.SemaphoreType.DMA((2, local)),
        ],
        out_shape=shapes,
        compiler_params=pltpu.CompilerParams(vmem_limit_bytes=GRANT),
        cost_estimate=cost(KERNEL_FLOPS, 2 * local * half * hidden),
    )(place, code, gate, near, far, own, other, after)


def shared_first_kernel(place, feed, own, other, _, part):
    quarter = own.shape[0]
    rows = part.shape[0] // 2
    here = pl.multiple_of(place[0] * quarter, quarter)
    there = pl.multiple_of((1 - place[0]) * quarter, quarter)
    total = dot(feed[0 : 2 * rows, pl.ds(here, quarter)], own[...])
    total += dot(feed[0 : 2 * rows, pl.ds(there, quarter)], other[...])
    for b in range(2):
        turn = place[1] if b == 0 else 1 - place[1]
        at = pl.ds(pl.multiple_of(turn * rows, rows), rows)
        part[at, :] = total[b * rows : (b + 1) * rows].astype(BF16)


def shared_second_kernel(place, near, far, own, other, _, out):
    quarter = own.shape[1]
    rows = near.shape[0] // 2
    here = pl.multiple_of(place[0] * quarter, quarter)
    there = pl.multiple_of((1 - place[0]) * quarter, quarter)
    hidden = jax.nn.gelu(near[...].astype(F32) + far[...].astype(F32)).astype(BF16)
    left, right = dot(hidden, own[...]), dot(hidden, other[...])
    for b in range(2):
        turn = place[1] if b == 0 else 1 - place[1]
        at = pl.ds(pl.multiple_of(turn * rows, rows), rows)
        out[at, pl.ds(here, quarter)] = left[b * rows : (b + 1) * rows]
        out[at, pl.ds(there, quarter)] = right[b * rows : (b + 1) * rows]


def exchanged_partials(tokens, expert_ids, gate_weights, expert_in, expert_out, shared_in, shared_out):
    rows, width = tokens.shape
    half = width // 2
    quarter = half // 2
    picks = expert_ids.shape[1]
    group = expert_in.shape[0]
    local = group // 2
    hidden = expert_in.shape[2]
    groups = lax.axis_size("expert")
    spot = lax.axis_index("dp")
    side, core = spot // 2, spot % 2
    lead = lax.axis_index("expert") * group + core * local
    place = jnp.stack([core, side, lead]).astype(jnp.int32)
    grant = pltpu.CompilerParams(vmem_limit_bytes=GRANT)

    mine, theirs, give_in = pl.pallas_call(
        norm_kernel,
        in_specs=[SMEM, VMEM, VMEM, VMEM, HBM],
        out_specs=[VMEM, VMEM, HBM],
        out_shape=[jax.ShapeDtypeStruct((rows + META, half), BF16)] * 2
        + [jax.ShapeDtypeStruct((local, quarter, hidden), BF16)],
        scratch_shapes=give_scratch(local, (quarter, hidden)),
        compiler_params=grant,
        cost_estimate=cost(KERNEL_FLOPS, 4 * rows * width),
        name="norm",
    )(place, tokens, expert_ids.T, gate_weights.T, expert_in)
    peer = swap(theirs, "dp", 2)
    other_in = swap(give_in, "dp", 1)
    give_out = pl.pallas_call(
        give_kernel,
        in_specs=[SMEM, HBM, ANY],
        out_specs=HBM,
        out_shape=jax.ShapeDtypeStruct((local, hidden, quarter), BF16),
        scratch_shapes=give_scratch(local, (hidden, quarter)),
        compiler_params=grant,
        cost_estimate=cost(KERNEL_FLOPS, 4 * local * hidden * quarter),
        name="give_out",
    )(place, expert_out, mine)
    other_shared_in = swap(shared_in, "dp", 1)
    other_out = swap(give_out, "dp", 1)
    other_shared_out = swap(shared_out, "dp", 1)

    unit = jnp.concatenate([mine[:rows], peer[:rows], mine[rows:], peer[rows:]], axis=0)
    feeds = {0: [unit]}
    far_groups = list(range(groups - 1, 0, -1))
    for g in far_groups:
        got = swap(unit, "expert", g)
        feeds[g] = [got, swap(got, "dp", 1)]
    feeds[groups] = [swap(unit, "dp", 1)]

    firsts = {}
    shared_part = shared_far = None
    sums = []
    last = give_out

    def first(g):
        nonlocal last
        part, code, gate = first_stage(feeds[g], place, expert_in, other_in, last, picks)
        firsts[g] = (part, code, gate, swap(part, "dp", 2))
        last = code

    def second(g):
        nonlocal last
        part, code, gate, far = firsts[g]
        keep, send = g != groups, g != 0
        outs = second_stage(
            len(feeds[g]), code, gate, part, far, place, expert_out, other_out, last,
            keep, send,
        )
        last = outs[0]
        if not send:
            sums.append(outs[0])
            return
        came = swap(outs[-1], "dp", 1).astype(F32)
        if keep:
            joined = (outs[0] + came).astype(BF16)
            came = swap(joined, "expert", g).astype(F32)
            last = joined
        sums.append(came)

    first(0)
    shared_part = pl.pallas_call(
        shared_first_kernel,
        in_specs=[SMEM, VMEM, VMEM, VMEM, ANY],
        out_specs=VMEM,
        out_shape=jax.ShapeDtypeStruct((2 * rows, hidden), BF16),
        cost_estimate=cost(KERNEL_FLOPS, 2 * half * hidden),
        compiler_params=grant,
        name="shared_first",
    )(place, unit, shared_in, other_shared_in, last)
    last = shared_part
    shared_far = swap(shared_part, "dp", 2)
    second(0)
    first(far_groups[0])
    shared = pl.pallas_call(
        shared_second_kernel,
        in_specs=[SMEM, VMEM, VMEM, VMEM, VMEM, ANY],
        out_specs=VMEM,
        out_shape=jax.ShapeDtypeStruct((2 * rows, half), F32),
        cost_estimate=cost(KERNEL_FLOPS, 2 * half * hidden),
        compiler_params=grant,
        name="shared_second",
    )(place, shared_part, shared_far, shared_out, other_shared_out, last)
    last = shared
    sums.append(shared)
    for g in far_groups[1:]:
        first(g)
    first(groups)
    for g in far_groups:
        second(g)
    second(groups)

    total = sum(sums[1:], sums[0])
    cross = swap(total[rows:].astype(BF16), "dp", 2).astype(F32)
    kept = total[:rows]
    low = side == 0
    added = jnp.concatenate([jnp.where(low, kept, cross), jnp.where(low, cross, kept)], axis=1)
    return (tokens.astype(F32) + added).astype(BF16)


def exchange_fits(mesh, tokens, expert_ids, expert_in):
    groups, sides = mesh.shape["expert"], mesh.shape["dp"]
    blocks = mesh.shape["sweep"] * groups
    rows, width = tokens.shape[0] // (blocks * sides), tokens.shape[1]
    return (
        sides == 4
        and expert_in.shape[0] % (blocks * 16) == 0
        and groups in (2, 4, 8)
        and rows % 128 == 0
        and width % 512 == 0
        and width // 2 >= 3 * rows
        and expert_ids.shape[1] <= 8
        and expert_in.shape[2] % 128 == 0
    )


def solution(mesh):
    rows = P(("sweep", "expert", "dp"), None)
    placed = (
        rows,
        rows,
        rows,
        P(("sweep", "expert"), "dp", None),
        P(("sweep", "expert"), None, "dp"),
        P(("sweep", "dp"), None),
        P("sweep", "dp"),
    )
    spread = functools.partial(
        jax.shard_map, mesh=mesh, in_specs=placed, out_specs=rows, check_vma=False
    )

    def program(*args):
        if not exchange_fits(mesh, args[0], args[1], args[3]):
            return spread(gathered_weights)(*args)
        step = spread(exchanged_partials)
        return step(*args)

    return program
```

```python
import functools

import jax
import jax.numpy as jnp
from jax import lax
from jax.experimental import pallas as pl
from jax.experimental.pallas import tpu as pltpu
from jax.sharding import PartitionSpec as P


CAP = 20
F32 = jnp.float32
BF16 = jnp.bfloat16
KERNEL_FLOPS = 10_000_000
META = 16


def layer_norm(tokens):
    values = tokens.astype(F32)
    center = values - jnp.mean(values, axis=-1, keepdims=True)
    spread = jnp.mean(center * center, axis=-1, keepdims=True)
    return (center * lax.rsqrt(spread + 1e-06)).astype(BF16)


def copy_slots(expert_ids, expert_count):
    expert_iota = jnp.arange(expert_count, dtype=jnp.int32)
    matches = (expert_ids[..., None] == expert_iota).astype(jnp.int32)
    per_token = jnp.sum(matches, axis=-2, dtype=jnp.int32)
    earlier = jnp.cumsum(per_token, axis=-2, dtype=jnp.int32) - per_token
    return jnp.sum(matches * earlier[..., None, :], axis=-1, dtype=jnp.int32)


def run_experts(shard_piece, weight_in, weight_out):
    pre_act = jnp.einsum("gesd,edf->gesf", shard_piece, weight_in, preferred_element_type=F32)
    hidden = jax.nn.gelu(pre_act).astype(BF16)
    return jnp.einsum("gesf,efd->gesd", hidden, weight_out, preferred_element_type=F32).astype(BF16)


def gathered_weights(tokens, expert_ids, gate_weights, expert_in, expert_out, shared_in, shared_out):
    row_count, model_width = tokens.shape
    pick_count = expert_ids.shape[1]
    local_count = expert_in.shape[0]
    group_count = lax.axis_size("expert")
    expert_total = local_count * group_count
    normed = layer_norm(tokens)
    full_in = lax.all_gather(expert_in, "dp", axis=1, tiled=True)
    full_out = lax.all_gather(expert_out, "dp", axis=2, tiled=True)
    slot_of = copy_slots(expert_ids, expert_total)
    positions = (expert_ids * CAP + slot_of).reshape(-1)
    copies = jnp.repeat(normed, pick_count, axis=0)
    outgoing = jnp.zeros((expert_total * CAP, model_width), BF16).at[positions].set(copies)
    outgoing = outgoing.reshape(group_count, local_count, CAP, model_width)
    received = lax.all_to_all(outgoing, "expert", split_axis=0, concat_axis=0, tiled=True)
    returned = lax.all_to_all(
        run_experts(received, full_in, full_out), "expert", split_axis=0, concat_axis=0, tiled=True
    )
    results = returned.reshape(expert_total * CAP, model_width)[positions].reshape(
        row_count, pick_count, model_width
    )
    routed = jnp.sum(results.astype(F32) * gate_weights[:, :, None], axis=1)
    shared_pre = jnp.dot(
        normed, lax.all_gather(shared_in, "dp", axis=0, tiled=True), preferred_element_type=F32
    )
    shared_hidden = jax.nn.gelu(shared_pre).astype(BF16)
    shared_result = jnp.dot(
        shared_hidden,
        lax.all_gather(shared_out, "dp", axis=1, tiled=True),
        preferred_element_type=F32,
    )
    return (tokens.astype(F32) + shared_result + routed).astype(BF16)


def dot(a, b):
    return jnp.dot(a, b, preferred_element_type=F32)


def swap(value, axis, mask):
    size = lax.axis_size(axis)
    return lax.ppermute(value, axis, [(i, i ^ mask) for i in range(size)])


def cost(flops, moved):
    return pl.CostEstimate(flops=int(flops), bytes_accessed=int(moved), transcendentals=0)


def half_copies(source, held, base, came):
    return [
        pltpu.make_async_copy(source.at[base + e], held.at[e], came.at[e])
        for e in range(held.shape[0])
    ]


def norm_kernel(place, tokens, ids, gates, source, mine, theirs, given, came):
    local = given.shape[0]
    copies = half_copies(source, given, (1 - place[0]) * local, came)
    for c in copies:
        c.start()
    rows, width = tokens.shape
    half = width // 2
    values = tokens[...].astype(F32)
    center = values - jnp.mean(values, axis=-1, keepdims=True)
    spread = jnp.mean(center * center, axis=-1, keepdims=True)
    normed = (center * lax.rsqrt(spread + 1e-06)).astype(BF16)
    low = place[1] == 0
    mine[0:rows, :] = jnp.where(low, normed[:, :half], normed[:, half:])
    theirs[0:rows, :] = jnp.where(low, normed[:, half:], normed[:, :half])
    gate = gates[...]
    high = gate.astype(BF16).astype(F32)
    rest = gate - high
    picks = ids.shape[0]
    spare = jnp.zeros((picks, half - 3 * rows), F32)
    table = jnp.concatenate([ids[...].astype(F32), high, rest, spare], axis=1)
    table = jnp.concatenate([table, jnp.zeros((META - picks, half), F32)], axis=0).astype(BF16)
    mine[rows : rows + META, :] = table
    theirs[rows : rows + META, :] = table
    for c in copies:
        c.wait()


def give_kernel(place, source, after, given, came):
    local = given.shape[0]
    copies = half_copies(source, given, (1 - place[0]) * local, came)
    for c in copies:
        c.start()
    for c in copies:
        c.wait()


def selection(codes, rows):
    count, tokens = codes.shape
    wanted = lax.broadcasted_iota(jnp.int32, (rows, tokens), 0).astype(F32)
    return [(wanted == codes[e : e + 1, :]).astype(F32) for e in range(count)]


def first_kernel(units, picks, load, place, *refs):
    feeds, refs = refs[:units], refs[units:]
    source, other, _, part, code, gate = refs[:6]
    own, (packed, made, left, *came) = (refs[6], refs[7:]) if load else (source, refs[6:])
    local, rows, half = packed.shape
    slots = rows // (2 * units)
    tokens = feeds[0].shape[0] // 2 - META
    if load:
        for c in half_copies(source, own, place[0] * local, came[0]):
            c.start()

    before = (
        lax.broadcasted_iota(jnp.int32, (tokens, tokens), 0)
        < lax.broadcasted_iota(jnp.int32, (tokens, tokens), 1)
    ).astype(F32).astype(BF16)
    expert = (lax.broadcasted_iota(jnp.int32, (local, tokens), 0) + place[2]).astype(F32)
    for u in range(units):
        for b in range(2):
            at = 2 * tokens + b * META
            table = feeds[u][at : at + META, 0 : 3 * tokens].astype(F32)
            named = jnp.zeros((local, tokens), F32)
            weight = jnp.zeros((local, tokens), F32)
            for k in range(picks):
                same = table[k : k + 1, 0:tokens] == expert
                value = table[k : k + 1, tokens : 2 * tokens] + table[k : k + 1, 2 * tokens :]
                named = jnp.where(same, 1.0, named)
                weight = jnp.where(same, value, weight)
            rank = dot(named.astype(BF16), before)
            turn = place[1] if b == 0 else 1 - place[1]
            base = ((2 * u + turn) * slots).astype(F32)
            column = (2 * u + b) * tokens
            code[:, column : column + tokens] = jnp.where(named > 0, rank + base, -1.0)
            gate[:, column : column + tokens] = weight
    pick = jnp.concatenate(selection(code[...], rows), axis=0).astype(BF16)
    wide = half // 3 if half % 384 == 0 else half
    for n in range(half // wide):
        columns = slice(n * wide, (n + 1) * wide)
        chosen = sum(
            dot(pick[:, 2 * u * tokens : 2 * (u + 1) * tokens], feeds[u][0 : 2 * tokens, columns])
            for u in range(units)
        )
        for e in range(local):
            packed[e, :, columns] = chosen[e * rows : (e + 1) * rows].astype(BF16)

    quarter = half // 2
    here = pl.multiple_of(place[0] * quarter, quarter)
    there = pl.multiple_of((1 - place[0]) * quarter, quarter)

    def put(e):
        return pltpu.make_async_copy(made.at[e], part.at[e], left.at[e])

    @pl.loop(0, local // 2)
    def _(pair):
        for e in (2 * pair, 2 * pair + 1):
            total = dot(packed[e, :, pl.ds(there, quarter)], other[e])
            if load:
                base = place[0] * local
                pltpu.make_async_copy(source.at[base + e], own.at[e], came[0].at[e]).wait()
            total += dot(packed[e, :, pl.ds(here, quarter)], own[e])
            made[e] = total.astype(BF16)
        for e in (2 * pair, 2 * pair + 1):
            put(e).start()

    @pl.loop(0, local)
    def _(e):
        put(e).wait()


def second_kernel(units, keep, send, load, place, *refs):
    code, gate, near, far, source, other, _ = refs[:7]
    shown = keep + send
    outs, refs = refs[7 : 7 + shown], refs[7 + shown :]
    own, (total, *came) = (refs[0], refs[1:]) if load else (source, refs)
    local = code.shape[0]
    rows = near.shape[1]
    half = total.shape[1]
    if load:
        for c in half_copies(source, own, place[0] * local, came[0]):
            c.start()
    quarter = half // 2
    here = pl.multiple_of(place[0] * quarter, quarter)
    there = pl.multiple_of((1 - place[0]) * quarter, quarter)
    wanted = lax.broadcasted_iota(jnp.int32, (rows, code.shape[1]), 0).astype(F32)

    @pl.loop(0, local // 2)
    def _(pair):
        for e in (2 * pair, 2 * pair + 1):
            same = wanted == code[pl.ds(e, 1), :]
            scale = jnp.sum(jnp.where(same, gate[pl.ds(e, 1), :], 0.0), axis=1, keepdims=True)
            hidden = jax.nn.gelu(near[e].astype(F32) + far[e].astype(F32)).astype(BF16)
            at = pl.ds(pl.multiple_of(e * rows, rows), rows)
            total[at, pl.ds(there, quarter)] = dot(hidden, other[e]) * scale
            if load:
                base = place[0] * local
                pltpu.make_async_copy(source.at[base + e], own.at[e], came[0].at[e]).wait()
            total[at, pl.ds(here, quarter)] = dot(hidden, own[e]) * scale

    pick = jnp.concatenate(selection(code[...], rows), axis=0).astype(BF16)
    wide = half // 3 if half % 384 == 0 else half
    count = code.shape[1] // units
    for n in range(half // wide):
        columns = slice(n * wide, (n + 1) * wide)
        summed = lax.dot_general(
            pick,
            total[:, columns].astype(BF16),
            (((0,), (0,)), ((), ())),
            preferred_element_type=F32,
        )
        slot = 0
        if keep:
            outs[slot][:, columns] = summed[0:count]
            slot += 1
        if send:
            outs[slot][:, columns] = summed[(units - 1) * count :].astype(BF16)


SMEM = pl.BlockSpec(memory_space=pltpu.SMEM)
VMEM = pl.BlockSpec(memory_space=pltpu.VMEM)
ANY = pl.BlockSpec(memory_space=pl.ANY)
HBM = pl.BlockSpec(memory_space=pltpu.HBM)
GRANT = 24 << 20
WEIGHT_GRANTS = {"norm": 46 << 20, "give": 42 << 20, "first": 40 << 20, "second": 36 << 20}


def granted(size=GRANT):
    return pltpu.CompilerParams(vmem_limit_bytes=size)


def first_stage(feeds, place, own, other, after, picks, load):
    units = len(feeds)
    local, quarter, hidden = other.shape
    half = 2 * quarter
    tokens = feeds[0].shape[0] // 2 - META
    rows = 2 * units * CAP
    table = jax.ShapeDtypeStruct((local, 2 * units * tokens), F32)
    return pl.pallas_call(
        functools.partial(first_kernel, units, picks, load),
        in_specs=[SMEM] + [VMEM] * units + [HBM if load else VMEM, VMEM, ANY],
        out_specs=[ANY, VMEM, VMEM] + [VMEM] * load,
        scratch_shapes=[
            pltpu.VMEM((local, rows, half), BF16),
            pltpu.VMEM((local, rows, hidden), BF16),
            pltpu.SemaphoreType.DMA((local,)),
        ]
        + [pltpu.SemaphoreType.DMA((local,))] * load,
        out_shape=[jax.ShapeDtypeStruct((local, rows, hidden), BF16), table, table]
        + [jax.ShapeDtypeStruct(other.shape, BF16)] * load,
        compiler_params=granted(WEIGHT_GRANTS["first"] if load else GRANT),
        cost_estimate=cost(KERNEL_FLOPS, 2 * local * half * hidden),
    )(place, *feeds, own, other, after)


def second_stage(units, code, gate, near, far, place, own, other, after, keep, send, load):
    local, hidden, quarter = other.shape
    half = 2 * quarter
    rows = near.shape[1]
    count = code.shape[1] // units
    shapes = []
    if keep:
        shapes.append(jax.ShapeDtypeStruct((count, half), F32))
    if send:
        shapes.append(jax.ShapeDtypeStruct((count, half), BF16))
    if load:
        shapes.append(jax.ShapeDtypeStruct(other.shape, BF16))
    return pl.pallas_call(
        functools.partial(second_kernel, units, keep, send, load),
        in_specs=[SMEM] + [VMEM] * 4 + [HBM if load else VMEM, VMEM, ANY],
        out_specs=[VMEM] * len(shapes),
        scratch_shapes=[pltpu.VMEM((local * rows, half), F32)]
        + [pltpu.SemaphoreType.DMA((local,))] * load,
        out_shape=shapes,
        compiler_params=granted(WEIGHT_GRANTS["second"] if load else GRANT),
        cost_estimate=cost(KERNEL_FLOPS, 2 * local * half * hidden),
    )(place, code, gate, near, far, own, other, after)


def shared_first_kernel(place, feed, own, other, _, part):
    quarter = own.shape[0]
    rows = part.shape[0] // 2
    here = pl.multiple_of(place[0] * quarter, quarter)
    there = pl.multiple_of((1 - place[0]) * quarter, quarter)
    total = dot(feed[0 : 2 * rows, pl.ds(here, quarter)], own[...])
    total += dot(feed[0 : 2 * rows, pl.ds(there, quarter)], other[...])
    for b in range(2):
        turn = place[1] if b == 0 else 1 - place[1]
        at = pl.ds(pl.multiple_of(turn * rows, rows), rows)
        part[at, :] = total[b * rows : (b + 1) * rows].astype(BF16)


def shared_second_kernel(place, near, far, own, other, _, out):
    quarter = own.shape[1]
    rows = near.shape[0] // 2
    here = pl.multiple_of(place[0] * quarter, quarter)
    there = pl.multiple_of((1 - place[0]) * quarter, quarter)
    hidden = jax.nn.gelu(near[...].astype(F32) + far[...].astype(F32)).astype(BF16)
    left, right = dot(hidden, own[...]), dot(hidden, other[...])
    for b in range(2):
        turn = place[1] if b == 0 else 1 - place[1]
        at = pl.ds(pl.multiple_of(turn * rows, rows), rows)
        out[at, pl.ds(here, quarter)] = left[b * rows : (b + 1) * rows]
        out[at, pl.ds(there, quarter)] = right[b * rows : (b + 1) * rows]


def exchanged_partials(tokens, expert_ids, gate_weights, expert_in, expert_out, shared_in, shared_out):
    rows, width = tokens.shape
    half = width // 2
    quarter = half // 2
    picks = expert_ids.shape[1]
    group = expert_in.shape[0]
    local = group // 2
    hidden = expert_in.shape[2]
    groups = lax.axis_size("expert")
    spot = lax.axis_index("dp")
    side, core = spot // 2, spot % 2
    lead = lax.axis_index("expert") * group + core * local
    place = jnp.stack([core, side, lead]).astype(jnp.int32)

    mine, theirs, give_in = pl.pallas_call(
        norm_kernel,
        in_specs=[SMEM, VMEM, VMEM, VMEM, HBM],
        out_specs=[VMEM, VMEM, VMEM],
        out_shape=[jax.ShapeDtypeStruct((rows + META, half), BF16)] * 2
        + [jax.ShapeDtypeStruct((local, quarter, hidden), BF16)],
        scratch_shapes=[pltpu.SemaphoreType.DMA((local,))],
        compiler_params=granted(WEIGHT_GRANTS["norm"]),
        cost_estimate=cost(KERNEL_FLOPS, 4 * rows * width),
        name="norm",
    )(place, tokens, expert_ids.T, gate_weights.T, expert_in)
    peer = swap(theirs, "dp", 2)
    other_in = swap(give_in, "dp", 1)
    give_out = pl.pallas_call(
        give_kernel,
        in_specs=[SMEM, HBM, ANY],
        out_specs=VMEM,
        out_shape=jax.ShapeDtypeStruct((local, hidden, quarter), BF16),
        scratch_shapes=[pltpu.SemaphoreType.DMA((local,))],
        compiler_params=granted(WEIGHT_GRANTS["give"]),
        cost_estimate=cost(KERNEL_FLOPS, 4 * local * hidden * quarter),
        name="give_out",
    )(place, expert_out, mine)
    other_shared_in = swap(shared_in, "dp", 1)
    other_out = swap(give_out, "dp", 1)
    other_shared_out = swap(shared_out, "dp", 1)

    unit = jnp.concatenate([mine[:rows], peer[:rows], mine[rows:], peer[rows:]], axis=0)
    far_groups = list(range(groups - 1, 1, -1))
    got = swap(unit, "expert", 1)
    feeds = {"own": [unit], "near": [got]}
    feeds["late"] = [swap(got, "dp", 1)]
    for g in far_groups:
        got = swap(unit, "expert", g)
        feeds[g] = [got, swap(got, "dp", 1)]
    feeds["twin"] = [swap(unit, "dp", 1)]

    firsts, kept, sums = {}, {}, []
    last, own_in, own_out = give_out, None, None

    def first(g):
        nonlocal last, own_in
        load = own_in is None
        part, code, gate, *held = first_stage(
            feeds[g], place, expert_in if load else own_in, other_in, last, picks,
            load,
        )
        firsts[g] = (part, code, gate, swap(part, "dp", 2))
        last = code
        own_in = held[0] if load else own_in

    def second(g):
        nonlocal last, own_out
        part, code, gate, far = firsts[g]
        load = own_out is None
        keep, send = g not in ("late", "twin"), g not in ("own", "near")
        outs = second_stage(
            len(feeds[g]), code, gate, part, far, place, expert_out if load else own_out,
            other_out, last, keep, send, load,
        )
        last = outs[0]
        own_out = outs[-1] if load else own_out
        if keep:
            kept[g] = outs[0]
        if not send:
            return
        came = swap(outs[keep], "dp", 1).astype(F32)
        if g != "twin":
            last = (kept.pop("near" if g == "late" else g) + came).astype(BF16)
            came = swap(last, "expert", 1 if g == "late" else g).astype(F32)
        sums.append(came)

    first("own")
    shared_part = pl.pallas_call(
        shared_first_kernel,
        in_specs=[SMEM, VMEM, VMEM, VMEM, ANY],
        out_specs=VMEM,
        out_shape=jax.ShapeDtypeStruct((2 * rows, hidden), BF16),
        cost_estimate=cost(KERNEL_FLOPS, 2 * half * hidden),
        compiler_params=granted(),
        name="shared_first",
    )(place, unit, shared_in, other_shared_in, last)
    last = shared_part
    shared_far = swap(shared_part, "dp", 2)
    first("near")
    second("own")
    for g in far_groups[:1]:
        first(g)
    shared = pl.pallas_call(
        shared_second_kernel,
        in_specs=[SMEM, VMEM, VMEM, VMEM, VMEM, ANY],
        out_specs=VMEM,
        out_shape=jax.ShapeDtypeStruct((2 * rows, half), F32),
        cost_estimate=cost(KERNEL_FLOPS, 2 * half * hidden),
        compiler_params=granted(),
        name="shared_second",
    )(place, shared_part, shared_far, shared_out, other_shared_out, last)
    last = shared
    second("near")
    for g in far_groups[1:]:
        first(g)
    first("late")
    first("twin")
    for g in far_groups + ["late", "twin"]:
        second(g)

    sums += [shared, kept["own"]]
    total = sum(sums[1:], sums[0])
    cross = swap(total[rows:].astype(BF16), "dp", 2).astype(F32)
    kept = total[:rows]
    low = side == 0
    added = jnp.concatenate([jnp.where(low, kept, cross), jnp.where(low, cross, kept)], axis=1)
    return (tokens.astype(F32) + added).astype(BF16)


def exchange_fits(mesh, tokens, expert_ids, expert_in):
    groups, sides = mesh.shape["expert"], mesh.shape["dp"]
    blocks = mesh.shape["sweep"] * groups
    rows, width = tokens.shape[0] // (blocks * sides), tokens.shape[1]
    return (
        sides == 4
        and expert_in.shape[0] % (blocks * 16) == 0
        and groups in (2, 4, 8)
        and rows % 128 == 0
        and width % 512 == 0
        and width // 2 >= 3 * rows
        and expert_ids.shape[1] <= 8
        and expert_in.shape[2] % 128 == 0
    )


def solution(mesh):
    rows = P(("sweep", "expert", "dp"), None)
    placed = (
        rows,
        rows,
        rows,
        P(("sweep", "expert"), "dp", None),
        P(("sweep", "expert"), None, "dp"),
        P(("sweep", "dp"), None),
        P("sweep", "dp"),
    )
    spread = functools.partial(
        jax.shard_map, mesh=mesh, in_specs=placed, out_specs=rows, check_vma=False
    )

    def program(*args):
        if not exchange_fits(mesh, args[0], args[1], args[3]):
            return spread(gathered_weights)(*args)
        step = spread(exchanged_partials)
        return step(*args)

    return program
```

```python
import functools

import jax
import jax.numpy as jnp
from jax import lax
from jax.experimental import pallas as pl
from jax.experimental.pallas import tpu as pltpu
from jax.sharding import PartitionSpec as P


CAP = 20
SWEEP, GROUP, SIDE = "sweep", "expert", "dp"
F32 = jnp.float32
BF16 = jnp.bfloat16
KERNEL_FLOPS = 10_000_000
META = 16


def layer_norm(tokens):
    values = tokens.astype(F32)
    center = values - jnp.mean(values, axis=-1, keepdims=True)
    spread = jnp.mean(center * center, axis=-1, keepdims=True)
    return (center * lax.rsqrt(spread + 1e-06)).astype(BF16)


def copy_slots(expert_ids, expert_count):
    expert_iota = jnp.arange(expert_count, dtype=jnp.int32)
    matches = (expert_ids[..., None] == expert_iota).astype(jnp.int32)
    per_token = jnp.sum(matches, axis=-2, dtype=jnp.int32)
    earlier = jnp.cumsum(per_token, axis=-2, dtype=jnp.int32) - per_token
    return jnp.sum(matches * earlier[..., None, :], axis=-1, dtype=jnp.int32)


def run_experts(shard_piece, weight_in, weight_out):
    pre_act = jnp.einsum("gesd,edf->gesf", shard_piece, weight_in, preferred_element_type=F32)
    hidden = jax.nn.gelu(pre_act).astype(BF16)
    return jnp.einsum("gesf,efd->gesd", hidden, weight_out, preferred_element_type=F32).astype(BF16)


def gathered_weights(tokens, expert_ids, gate_weights, expert_in, expert_out, shared_in, shared_out):
    row_count, model_width = tokens.shape
    pick_count = expert_ids.shape[1]
    local_count = expert_in.shape[0]
    group_count = lax.axis_size(GROUP)
    expert_total = local_count * group_count
    normed = layer_norm(tokens)
    full_in = lax.all_gather(expert_in, SIDE, axis=1, tiled=True)
    full_out = lax.all_gather(expert_out, SIDE, axis=2, tiled=True)
    slot_of = copy_slots(expert_ids, expert_total)
    positions = (expert_ids * CAP + slot_of).reshape(-1)
    copies = jnp.repeat(normed, pick_count, axis=0)
    outgoing = jnp.zeros((expert_total * CAP, model_width), BF16).at[positions].set(copies)
    outgoing = outgoing.reshape(group_count, local_count, CAP, model_width)
    received = lax.all_to_all(outgoing, GROUP, split_axis=0, concat_axis=0, tiled=True)
    returned = lax.all_to_all(
        run_experts(received, full_in, full_out), GROUP, split_axis=0, concat_axis=0, tiled=True
    )
    results = returned.reshape(expert_total * CAP, model_width)[positions].reshape(
        row_count, pick_count, model_width
    )
    routed = jnp.sum(results.astype(F32) * gate_weights[:, :, None], axis=1)
    shared_pre = jnp.dot(
        normed, lax.all_gather(shared_in, SIDE, axis=0, tiled=True), preferred_element_type=F32
    )
    shared_hidden = jax.nn.gelu(shared_pre).astype(BF16)
    shared_result = jnp.dot(
        shared_hidden,
        lax.all_gather(shared_out, SIDE, axis=1, tiled=True),
        preferred_element_type=F32,
    )
    return (tokens.astype(F32) + shared_result + routed).astype(BF16)


def dot(a, b):
    return jnp.dot(a, b, preferred_element_type=F32)


def cost(flops, moved):
    return pl.CostEstimate(flops=int(flops), bytes_accessed=int(moved), transcendentals=0)


def half_copies(source, held, base, came):
    return [
        pltpu.make_async_copy(source.at[base + e], held.at[e], came.at[e])
        for e in range(held.shape[0])
    ]


def norm_kernel(place, tokens, ids, gates, _, mine, theirs):
    rows, width = tokens.shape
    half = width // 2
    values = tokens[...].astype(F32)
    center = values - jnp.mean(values, axis=-1, keepdims=True)
    spread = jnp.mean(center * center, axis=-1, keepdims=True)
    normed = (center * lax.rsqrt(spread + 1e-06)).astype(BF16)
    low = place[1] == 0
    mine[0:rows, :] = jnp.where(low, normed[:, :half], normed[:, half:])
    theirs[0:rows, :] = jnp.where(low, normed[:, half:], normed[:, :half])
    gate = gates[...]
    high = gate.astype(BF16).astype(F32)
    rest = gate - high
    picks = ids.shape[0]
    spare = jnp.zeros((picks, half - 3 * rows), F32)
    table = jnp.concatenate([ids[...].astype(F32), high, rest, spare], axis=1)
    table = jnp.concatenate([table, jnp.zeros((META - picks, half), F32)], axis=0).astype(BF16)
    mine[rows : rows + META, :] = table
    theirs[rows : rows + META, :] = table


def give_kernel(place, source, after, given, came):
    local = given.shape[0]
    copies = half_copies(source, given, (1 - place[0]) * local, came)
    for c in copies:
        c.start()
    for c in copies:
        c.wait()


def selection(codes, rows):
    count, tokens = codes.shape
    wanted = lax.broadcasted_iota(jnp.int32, (rows, tokens), 0).astype(F32)
    return [(wanted == codes[e : e + 1, :]).astype(F32) for e in range(count)]


def first_kernel(units, picks, load, place, *refs):
    feeds, refs = refs[:units], refs[units:]
    source, other, _, part, code, gate = refs[:6]
    own, (packed, *came) = (refs[6], refs[7:]) if load else (source, refs[6:])
    local, rows, half = packed.shape
    slots = rows // (2 * units)
    tokens = feeds[0].shape[0] // 2 - META
    if load:
        for c in half_copies(source, own, place[0] * local, came[0]):
            c.start()

    before = (
        lax.broadcasted_iota(jnp.int32, (tokens, tokens), 0)
        < lax.broadcasted_iota(jnp.int32, (tokens, tokens), 1)
    ).astype(F32).astype(BF16)
    expert = (lax.broadcasted_iota(jnp.int32, (local, tokens), 0) + place[2]).astype(F32)
    for u in range(units):
        for b in range(2):
            at = 2 * tokens + b * META
            table = feeds[u][at : at + META, 0 : 3 * tokens].astype(F32)
            named = jnp.zeros((local, tokens), F32)
            weight = jnp.zeros((local, tokens), F32)
            for k in range(picks):
                same = table[k : k + 1, 0:tokens] == expert
                value = table[k : k + 1, tokens : 2 * tokens] + table[k : k + 1, 2 * tokens :]
                named = jnp.where(same, 1.0, named)
                weight = jnp.where(same, value, weight)
            rank = dot(named.astype(BF16), before)
            turn = place[1] if b == 0 else 1 - place[1]
            base = ((2 * u + turn) * slots).astype(F32)
            column = (2 * u + b) * tokens
            code[:, column : column + tokens] = jnp.where(named > 0, rank + base, -1.0)
            gate[:, column : column + tokens] = weight
    pick = jnp.concatenate(selection(code[...], rows), axis=0).astype(BF16)
    wide = half // 3 if half % 384 == 0 else half
    for n in range(half // wide):
        columns = slice(n * wide, (n + 1) * wide)
        chosen = sum(
            dot(pick[:, 2 * u * tokens : 2 * (u + 1) * tokens], feeds[u][0 : 2 * tokens, columns])
            for u in range(units)
        )
        for e in range(local):
            packed[e, :, columns] = chosen[e * rows : (e + 1) * rows].astype(BF16)

    quarter = half // 2
    here = pl.multiple_of(place[0] * quarter, quarter)
    there = pl.multiple_of((1 - place[0]) * quarter, quarter)

    @pl.loop(0, local // 2)
    def _(pair):
        for e in (2 * pair, 2 * pair + 1):
            total = dot(packed[e, :, pl.ds(there, quarter)], other[e])
            if load:
                base = place[0] * local
                pltpu.make_async_copy(source.at[base + e], own.at[e], came[0].at[e]).wait()
            total += dot(packed[e, :, pl.ds(here, quarter)], own[e])
            part[e] = total.astype(BF16)


def second_kernel(units, keep, send, load, place, *refs):
    code, gate, near, far, source, other, _ = refs[:7]
    shown = keep + send
    outs, refs = refs[7 : 7 + shown], refs[7 + shown :]
    own, (total, *came) = (refs[0], refs[1:]) if load else (source, refs)
    local = code.shape[0]
    rows = near.shape[1]
    half = total.shape[1]
    if load:
        for c in half_copies(source, own, place[0] * local, came[0]):
            c.start()
    quarter = half // 2
    here = pl.multiple_of(place[0] * quarter, quarter)
    there = pl.multiple_of((1 - place[0]) * quarter, quarter)
    wanted = lax.broadcasted_iota(jnp.int32, (rows, code.shape[1]), 0).astype(F32)

    @pl.loop(0, local // 2)
    def _(pair):
        for e in (2 * pair, 2 * pair + 1):
            same = wanted == code[pl.ds(e, 1), :]
            scale = jnp.sum(jnp.where(same, gate[pl.ds(e, 1), :], 0.0), axis=1, keepdims=True)
            hidden = jax.nn.gelu(near[e].astype(F32) + far[e].astype(F32)).astype(BF16)
            at = pl.ds(pl.multiple_of(e * rows, rows), rows)
            total[at, pl.ds(there, quarter)] = dot(hidden, other[e]) * scale
            if load:
                base = place[0] * local
                pltpu.make_async_copy(source.at[base + e], own.at[e], came[0].at[e]).wait()
            total[at, pl.ds(here, quarter)] = dot(hidden, own[e]) * scale

    pick = jnp.concatenate(selection(code[...], rows), axis=0).astype(BF16)
    wide = half // 3 if half % 384 == 0 else half
    count = code.shape[1] // units
    for n in range(half // wide):
        columns = slice(n * wide, (n + 1) * wide)
        summed = lax.dot_general(
            pick,
            total[:, columns].astype(BF16),
            (((0,), (0,)), ((), ())),
            preferred_element_type=F32,
        )
        slot = 0
        if keep:
            outs[slot][:, columns] = summed[0:count]
            slot += 1
        if send:
            outs[slot][:, columns] = summed[(units - 1) * count :].astype(BF16)


SMEM = pl.BlockSpec(memory_space=pltpu.SMEM)
VMEM = pl.BlockSpec(memory_space=pltpu.VMEM)
ANY = pl.BlockSpec(memory_space=pl.ANY)
HBM = pl.BlockSpec(memory_space=pltpu.HBM)
GRANT = 24 << 20
GIVE_GRANTS = (46 << 20, 42 << 20)
FIRST_GRANT = 40 << 20
SECOND_GRANT = 36 << 20


def granted(size=GRANT):
    return pltpu.CompilerParams(vmem_limit_bytes=size)


def first_stage(feeds, place, own, other, after, picks, load):
    units = len(feeds)
    local, quarter, hidden = other.shape
    half = 2 * quarter
    tokens = feeds[0].shape[0] // 2 - META
    rows = 2 * units * CAP
    table = jax.ShapeDtypeStruct((local, 2 * units * tokens), F32)
    return pl.pallas_call(
        functools.partial(first_kernel, units, picks, load),
        in_specs=[SMEM] + [VMEM] * units + [HBM if load else VMEM, VMEM, ANY],
        out_specs=[VMEM] * (3 + load),
        scratch_shapes=[pltpu.VMEM((local, rows, half), BF16)]
        + [pltpu.SemaphoreType.DMA((local,))] * load,
        out_shape=[jax.ShapeDtypeStruct((local, rows, hidden), BF16), table, table]
        + [jax.ShapeDtypeStruct(other.shape, BF16)] * load,
        compiler_params=granted(FIRST_GRANT if load else GRANT),
        cost_estimate=cost(KERNEL_FLOPS, 2 * local * half * hidden),
    )(place, *feeds, own, other, after)


def second_stage(units, code, gate, near, far, place, own, other, after, keep, send, load):
    local, hidden, quarter = other.shape
    half = 2 * quarter
    rows = near.shape[1]
    count = code.shape[1] // units
    shapes = []
    if keep:
        shapes.append(jax.ShapeDtypeStruct((count, half), F32))
    if send:
        shapes.append(jax.ShapeDtypeStruct((count, half), BF16))
    if load:
        shapes.append(jax.ShapeDtypeStruct(other.shape, BF16))
    return pl.pallas_call(
        functools.partial(second_kernel, units, keep, send, load),
        in_specs=[SMEM] + [VMEM] * 4 + [HBM if load else VMEM, VMEM, ANY],
        out_specs=[VMEM] * len(shapes),
        scratch_shapes=[pltpu.VMEM((local * rows, half), F32)]
        + [pltpu.SemaphoreType.DMA((local,))] * load,
        out_shape=shapes,
        compiler_params=granted(SECOND_GRANT if load else GRANT),
        cost_estimate=cost(KERNEL_FLOPS, 2 * local * half * hidden),
    )(place, code, gate, near, far, own, other, after)


def shared_first_kernel(place, feed, own, other, _, part):
    quarter = own.shape[0]
    rows = part.shape[0] // 2
    here = pl.multiple_of(place[0] * quarter, quarter)
    there = pl.multiple_of((1 - place[0]) * quarter, quarter)
    total = dot(feed[0 : 2 * rows, pl.ds(here, quarter)], own[...])
    total += dot(feed[0 : 2 * rows, pl.ds(there, quarter)], other[...])
    for b in range(2):
        turn = place[1] if b == 0 else 1 - place[1]
        at = pl.ds(pl.multiple_of(turn * rows, rows), rows)
        part[at, :] = total[b * rows : (b + 1) * rows].astype(BF16)


def shared_second_kernel(place, near, far, own, other, _, out):
    quarter = own.shape[1]
    rows = near.shape[0] // 2
    here = pl.multiple_of(place[0] * quarter, quarter)
    there = pl.multiple_of((1 - place[0]) * quarter, quarter)
    hidden = jax.nn.gelu(near[...].astype(F32) + far[...].astype(F32)).astype(BF16)
    left, right = dot(hidden, own[...]), dot(hidden, other[...])
    for b in range(2):
        turn = place[1] if b == 0 else 1 - place[1]
        at = pl.ds(pl.multiple_of(turn * rows, rows), rows)
        out[at, pl.ds(here, quarter)] = left[b * rows : (b + 1) * rows]
        out[at, pl.ds(there, quarter)] = right[b * rows : (b + 1) * rows]


def give_stage(place, source, after, grant):
    shape = (source.shape[0] // 2, *source.shape[1:])
    return pl.pallas_call(
        give_kernel,
        in_specs=[SMEM, HBM, ANY],
        out_specs=VMEM,
        out_shape=jax.ShapeDtypeStruct(shape, BF16),
        scratch_shapes=[pltpu.SemaphoreType.DMA(shape[:1])],
        compiler_params=granted(grant),
        cost_estimate=cost(KERNEL_FLOPS, 4 * shape[0] * shape[1] * shape[2]),
    )(place, source, after)


def kernel(body, after, shapes, place, *args):
    return pl.pallas_call(
        body,
        in_specs=[SMEM] + [VMEM] * len(args) + [ANY],
        out_specs=[VMEM] * len(shapes),
        out_shape=shapes,
        compiler_params=granted(),
        cost_estimate=cost(KERNEL_FLOPS, 1 << 20),
    )(place, *args, after)


def exchanged_partials(tokens, expert_ids, gate_weights, expert_in, expert_out, shared_in, shared_out):
    rows, width = tokens.shape
    half = width // 2
    picks = expert_ids.shape[1]
    group = expert_in.shape[0]
    local = group // 2
    hidden = expert_in.shape[2]
    groups = lax.axis_size(GROUP)
    spot = lax.axis_index(SIDE)
    side, core = spot // 2, spot % 2
    lead = lax.axis_index(GROUP) * group + core * local
    place = jnp.stack([core, side, lead]).astype(jnp.int32)

    def swap(value, axis, mask):
        return lax.ppermute(value, axis, [(i, i ^ mask) for i in range(lax.axis_size(axis))])

    def cross(value):
        return swap(value, SIDE, 2)

    def share(value):
        return swap(value, SIDE, 1)

    give_in = give_stage(place, expert_in, place, GIVE_GRANTS[0])
    other_in = share(give_in)
    block = jax.ShapeDtypeStruct((rows + META, half), BF16)
    mine, theirs = kernel(
        norm_kernel, give_in, [block] * 2,
        place, tokens, expert_ids.T, gate_weights.T,
    )
    peer = cross(theirs)
    give_out = give_stage(place, expert_out, mine, GIVE_GRANTS[1])
    other_shared_in = share(shared_in)
    other_out = share(give_out)
    other_shared_out = share(shared_out)

    unit = jnp.concatenate([mine[:rows], peer[:rows], mine[rows:], peer[rows:]], axis=0)
    far = far_groups(groups)
    near = swap(unit, GROUP, 1)
    feeds = {"o": [unit], "n": [near], "l": [share(near)], "t": [share(unit)]}
    for g in far:
        if g % 2:
            got = swap(unit, GROUP, g)
        else:
            got = swap(feeds[str(g + 1)][0], GROUP, 1)
        feeds[str(g)] = [got, share(got)]

    firsts, kept, sums = {}, {}, []
    last, own_in, own_out = give_out, None, None

    def first(g):
        nonlocal last, own_in
        load = own_in is None
        part, code, gate, *held = first_stage(
            feeds[g], place, expert_in if load else own_in, other_in, last, picks,
            load,
        )
        firsts[g] = (part, code, gate, cross(part))
        last = code
        own_in = held[0] if load else own_in

    def second(g):
        nonlocal last, own_out
        part, code, gate, across = firsts[g]
        load = own_out is None
        keep, send = g not in "lt", g not in "on"
        outs = second_stage(
            len(feeds[g]), code, gate, part, across, place, expert_out if load else own_out,
            other_out, last, keep, send, load,
        )
        last = outs[0]
        own_out = outs[-1] if load else own_out
        if keep:
            kept[g] = outs[0]
        if not send:
            return
        came = share(outs[keep]).astype(F32)
        if g != "t":
            last = (kept.pop("n" if g == "l" else g) + came).astype(BF16)
            came = swap(last, GROUP, 1 if g == "l" else int(g)).astype(F32)
        sums.append(came)

    first("o")
    (shared_part,) = kernel(
        shared_first_kernel, last,
        [jax.ShapeDtypeStruct((2 * rows, hidden), BF16)],
        place, unit, shared_in, other_shared_in,
    )
    last = shared_part
    shared_far = cross(shared_part)
    first("n")
    second("o")
    for g in far[:1]:
        first(str(g))
    (shared,) = kernel(
        shared_second_kernel, last,
        [jax.ShapeDtypeStruct((2 * rows, half), F32)],
        place, shared_part, shared_far, shared_out, other_shared_out,
    )
    last = shared
    second("n")
    for g in far[1:]:
        first(str(g))
    first("l")
    first("t")
    for g in [*map(str, far), "l", "t"]:
        second(g)

    total = sum(sums, shared + kept["o"])
    crossed = cross(total[rows:].astype(BF16)).astype(F32)
    stay = total[:rows]
    low = side == 0
    added = jnp.concatenate([jnp.where(low, stay, crossed), jnp.where(low, crossed, stay)], axis=1)
    return (tokens.astype(F32) + added).astype(BF16)


def exchange_fits(mesh, tokens, expert_ids, expert_in):
    groups, sides = mesh.shape[GROUP], mesh.shape[SIDE]
    blocks = mesh.shape[SWEEP] * groups
    rows, width = tokens.shape[0] // (blocks * sides), tokens.shape[1]
    return (
        sides == 4
        and expert_in.shape[0] % (blocks * 16) == 0
        and groups in (2, 4, 8)
        and rows % 128 == 0
        and width % 512 == 0
        and width // 2 >= 3 * rows
        and expert_ids.shape[1] <= 8
        and expert_in.shape[2] % 128 == 0
    )


def far_groups(groups):
    return list(range(groups - 1, 1, -1))


def solution(mesh):
    rows = P((SWEEP, GROUP, SIDE), None)
    placed = (
        rows,
        rows,
        rows,
        P((SWEEP, GROUP), SIDE, None),
        P((SWEEP, GROUP), None, SIDE),
        P((SWEEP, SIDE), None),
        P(SWEEP, SIDE),
    )
    spread = functools.partial(
        jax.shard_map, mesh=mesh, in_specs=placed, out_specs=rows, check_vma=False
    )

    def program(*args):
        if not exchange_fits(mesh, args[0], args[1], args[3]):
            return spread(gathered_weights)(*args)
        step = spread(exchanged_partials)
        return step(*args)

    return program
```

```python
import functools

import jax
import jax.numpy as jnp
from jax import lax
from jax.experimental import pallas as pl
from jax.experimental.pallas import tpu as pltpu
from jax.sharding import PartitionSpec as P


CAP = 20
SWEEP, GROUP, SIDE = "sweep", "expert", "dp"
F32 = jnp.float32
BF16 = jnp.bfloat16
KERNEL_FLOPS = 10_000_000
META = 16


def layer_norm(tokens):
    values = tokens.astype(F32)
    center = values - jnp.mean(values, axis=-1, keepdims=True)
    spread = jnp.mean(center * center, axis=-1, keepdims=True)
    return (center * lax.rsqrt(spread + 1e-06)).astype(BF16)


def copy_slots(expert_ids, expert_count):
    expert_iota = jnp.arange(expert_count, dtype=jnp.int32)
    matches = (expert_ids[..., None] == expert_iota).astype(jnp.int32)
    per_token = jnp.sum(matches, axis=-2, dtype=jnp.int32)
    earlier = jnp.cumsum(per_token, axis=-2, dtype=jnp.int32) - per_token
    return jnp.sum(matches * earlier[..., None, :], axis=-1, dtype=jnp.int32)


def run_experts(shard_piece, weight_in, weight_out):
    pre_act = jnp.einsum("gesd,edf->gesf", shard_piece, weight_in, preferred_element_type=F32)
    hidden = jax.nn.gelu(pre_act).astype(BF16)
    return jnp.einsum("gesf,efd->gesd", hidden, weight_out, preferred_element_type=F32).astype(BF16)


def gathered_weights(tokens, expert_ids, gate_weights, expert_in, expert_out, shared_in, shared_out):
    row_count, model_width = tokens.shape
    pick_count = expert_ids.shape[1]
    local_count = expert_in.shape[0]
    group_count = lax.axis_size(GROUP)
    expert_total = local_count * group_count
    normed = layer_norm(tokens)
    full_in = lax.all_gather(expert_in, SIDE, axis=1, tiled=True)
    full_out = lax.all_gather(expert_out, SIDE, axis=2, tiled=True)
    slot_of = copy_slots(expert_ids, expert_total)
    positions = (expert_ids * CAP + slot_of).reshape(-1)
    copies = jnp.repeat(normed, pick_count, axis=0)
    outgoing = jnp.zeros((expert_total * CAP, model_width), BF16).at[positions].set(copies)
    outgoing = outgoing.reshape(group_count, local_count, CAP, model_width)
    received = lax.all_to_all(outgoing, GROUP, split_axis=0, concat_axis=0, tiled=True)
    returned = lax.all_to_all(
        run_experts(received, full_in, full_out), GROUP, split_axis=0, concat_axis=0, tiled=True
    )
    results = returned.reshape(expert_total * CAP, model_width)[positions].reshape(
        row_count, pick_count, model_width
    )
    routed = jnp.sum(results.astype(F32) * gate_weights[:, :, None], axis=1)
    shared_pre = jnp.dot(
        normed, lax.all_gather(shared_in, SIDE, axis=0, tiled=True), preferred_element_type=F32
    )
    shared_hidden = jax.nn.gelu(shared_pre).astype(BF16)
    shared_result = jnp.dot(
        shared_hidden,
        lax.all_gather(shared_out, SIDE, axis=1, tiled=True),
        preferred_element_type=F32,
    )
    return (tokens.astype(F32) + shared_result + routed).astype(BF16)


def dot(a, b):
    return jnp.dot(a, b, preferred_element_type=F32)


def cost(flops, moved):
    return pl.CostEstimate(flops=int(flops), bytes_accessed=int(moved), transcendentals=0)


def half_copies(source, held, base, came):
    return [
        pltpu.make_async_copy(source.at[base + e], held.at[e], came.at[e])
        for e in range(held.shape[0])
    ]


def norm_kernel(place, tokens, ids, gates, _, mine, theirs):
    rows, width = tokens.shape
    half = width // 2
    values = tokens[...].astype(F32)
    center = values - jnp.mean(values, axis=-1, keepdims=True)
    spread = jnp.mean(center * center, axis=-1, keepdims=True)
    normed = (center * lax.rsqrt(spread + 1e-06)).astype(BF16)
    low = place[1] == 0
    mine[0:rows, :] = jnp.where(low, normed[:, :half], normed[:, half:])
    theirs[0:rows, :] = jnp.where(low, normed[:, half:], normed[:, :half])
    gate = gates[...]
    high = gate.astype(BF16).astype(F32)
    rest = gate - high
    picks = ids.shape[0]
    spare = jnp.zeros((picks, half - 3 * rows), F32)
    table = jnp.concatenate([ids[...].astype(F32), high, rest, spare], axis=1)
    table = jnp.concatenate([table, jnp.zeros((META - picks, half), F32)], axis=0).astype(BF16)
    mine[rows : rows + META, :] = table
    theirs[rows : rows + META, :] = table


def take_kernel(own, place, source, after, taken, came):
    local = taken.shape[0]
    copies = half_copies(source, taken, (place[0] if own else 1 - place[0]) * local, came)
    for c in copies:
        c.start()
    for c in copies:
        c.wait()


def selection(codes, rows):
    count, tokens = codes.shape
    wanted = lax.broadcasted_iota(jnp.int32, (rows, tokens), 0).astype(F32)
    return [(wanted == codes[e : e + 1, :]).astype(F32) for e in range(count)]


def first_kernel(units, picks, place, *refs):
    feeds, refs = refs[:units], refs[units:]
    own, other, _, part, code, gate, packed = refs
    local, rows, half = packed.shape
    slots = rows // (2 * units)
    tokens = feeds[0].shape[0] // 2 - META
    before = (
        lax.broadcasted_iota(jnp.int32, (tokens, tokens), 0)
        < lax.broadcasted_iota(jnp.int32, (tokens, tokens), 1)
    ).astype(F32).astype(BF16)
    expert = (lax.broadcasted_iota(jnp.int32, (local, tokens), 0) + place[2]).astype(F32)
    for u in range(units):
        for b in range(2):
            at = 2 * tokens + b * META
            table = feeds[u][at : at + META, 0 : 3 * tokens].astype(F32)
            named = jnp.zeros((local, tokens), F32)
            weight = jnp.zeros((local, tokens), F32)
            for k in range(picks):
                same = table[k : k + 1, 0:tokens] == expert
                value = table[k : k + 1, tokens : 2 * tokens] + table[k : k + 1, 2 * tokens :]
                named = jnp.where(same, 1.0, named)
                weight = jnp.where(same, value, weight)
            rank = dot(named.astype(BF16), before)
            turn = place[1] if b == 0 else 1 - place[1]
            base = ((2 * u + turn) * slots).astype(F32)
            column = (2 * u + b) * tokens
            code[:, column : column + tokens] = jnp.where(named > 0, rank + base, -1.0)
            gate[:, column : column + tokens] = weight
    pick = jnp.concatenate(selection(code[...], rows), axis=0).astype(BF16)
    wide = half // 3 if half % 384 == 0 else half
    for n in range(half // wide):
        columns = slice(n * wide, (n + 1) * wide)
        chosen = sum(
            dot(pick[:, 2 * u * tokens : 2 * (u + 1) * tokens], feeds[u][0 : 2 * tokens, columns])
            for u in range(units)
        )
        for e in range(local):
            packed[e, :, columns] = chosen[e * rows : (e + 1) * rows].astype(BF16)

    quarter = half // 2
    here = pl.multiple_of(place[0] * quarter, quarter)
    there = pl.multiple_of((1 - place[0]) * quarter, quarter)

    @pl.loop(0, local // 2)
    def _(pair):
        for e in (2 * pair, 2 * pair + 1):
            total = dot(packed[e, :, pl.ds(here, quarter)], own[e])
            total += dot(packed[e, :, pl.ds(there, quarter)], other[e])
            part[e] = total.astype(BF16)


def second_kernel(units, keep, send, load, place, *refs):
    code, gate, near, far, source, other, _ = refs[:7]
    shown = keep + send
    outs, refs = refs[7 : 7 + shown], refs[7 + shown :]
    own, (total, *came) = (refs[0], refs[1:]) if load else (source, refs)
    local = code.shape[0]
    rows = near.shape[1]
    half = total.shape[1]
    if load:
        for c in half_copies(source, own, place[0] * local, came[0]):
            c.start()
    quarter = half // 2
    here = pl.multiple_of(place[0] * quarter, quarter)
    there = pl.multiple_of((1 - place[0]) * quarter, quarter)
    wanted = lax.broadcasted_iota(jnp.int32, (rows, code.shape[1]), 0).astype(F32)

    @pl.loop(0, local // 2)
    def _(pair):
        for e in (2 * pair, 2 * pair + 1):
            same = wanted == code[pl.ds(e, 1), :]
            scale = jnp.sum(jnp.where(same, gate[pl.ds(e, 1), :], 0.0), axis=1, keepdims=True)
            hidden = jax.nn.gelu(near[e].astype(F32) + far[e].astype(F32)).astype(BF16)
            at = pl.ds(pl.multiple_of(e * rows, rows), rows)
            total[at, pl.ds(there, quarter)] = dot(hidden, other[e]) * scale
            if load:
                base = place[0] * local
                pltpu.make_async_copy(source.at[base + e], own.at[e], came[0].at[e]).wait()
            total[at, pl.ds(here, quarter)] = dot(hidden, own[e]) * scale

    pick = jnp.concatenate(selection(code[...], rows), axis=0).astype(BF16)
    wide = half // 3 if half % 384 == 0 else half
    count = code.shape[1] // units
    for n in range(half // wide):
        columns = slice(n * wide, (n + 1) * wide)
        summed = lax.dot_general(
            pick,
            total[:, columns].astype(BF16),
            (((0,), (0,)), ((), ())),
            preferred_element_type=F32,
        )
        slot = 0
        if keep:
            outs[slot][:, columns] = summed[0:count]
            slot += 1
        if send:
            outs[slot][:, columns] = summed[(units - 1) * count :].astype(BF16)


SMEM = pl.BlockSpec(memory_space=pltpu.SMEM)
VMEM = pl.BlockSpec(memory_space=pltpu.VMEM)
ANY = pl.BlockSpec(memory_space=pl.ANY)
HBM = pl.BlockSpec(memory_space=pltpu.HBM)
GRANT = 24 << 20
GIVE_GRANTS = (46 << 20, 42 << 20, 44 << 20)
SECOND_GRANT = 36 << 20


def granted(size=GRANT):
    return pltpu.CompilerParams(vmem_limit_bytes=size)


def first_stage(feeds, place, own, other, after, picks):
    units = len(feeds)
    local, quarter, hidden = other.shape
    half = 2 * quarter
    tokens = feeds[0].shape[0] // 2 - META
    rows = 2 * units * CAP
    table = jax.ShapeDtypeStruct((local, 2 * units * tokens), F32)
    return pl.pallas_call(
        functools.partial(first_kernel, units, picks),
        in_specs=[SMEM] + [VMEM] * (units + 2) + [ANY],
        out_specs=[VMEM] * 3,
        scratch_shapes=[pltpu.VMEM((local, rows, half), BF16)],
        out_shape=[jax.ShapeDtypeStruct((local, rows, hidden), BF16), table, table],
        compiler_params=granted(),
        cost_estimate=cost(KERNEL_FLOPS, 2 * local * half * hidden),
    )(place, *feeds, own, other, after)


def second_stage(units, code, gate, near, far, place, own, other, after, keep, send, load):
    local, hidden, quarter = other.shape
    half = 2 * quarter
    rows = near.shape[1]
    count = code.shape[1] // units
    shapes = []
    if keep:
        shapes.append(jax.ShapeDtypeStruct((count, half), F32))
    if send:
        shapes.append(jax.ShapeDtypeStruct((count, half), BF16))
    if load:
        shapes.append(jax.ShapeDtypeStruct(other.shape, BF16))
    return pl.pallas_call(
        functools.partial(second_kernel, units, keep, send, load),
        in_specs=[SMEM] + [VMEM] * 4 + [HBM if load else VMEM, VMEM, ANY],
        out_specs=[VMEM] * len(shapes),
        scratch_shapes=[pltpu.VMEM((local * rows, half), F32)]
        + [pltpu.SemaphoreType.DMA((local,))] * load,
        out_shape=shapes,
        compiler_params=granted(SECOND_GRANT if load else GRANT),
        cost_estimate=cost(KERNEL_FLOPS, 2 * local * half * hidden),
    )(place, code, gate, near, far, own, other, after)


def shared_first_kernel(place, feed, own, other, _, part):
    quarter = own.shape[0]
    rows = part.shape[0] // 2
    here = pl.multiple_of(place[0] * quarter, quarter)
    there = pl.multiple_of((1 - place[0]) * quarter, quarter)
    total = dot(feed[0 : 2 * rows, pl.ds(here, quarter)], own[...])
    total += dot(feed[0 : 2 * rows, pl.ds(there, quarter)], other[...])
    for b in range(2):
        turn = place[1] if b == 0 else 1 - place[1]
        at = pl.ds(pl.multiple_of(turn * rows, rows), rows)
        part[at, :] = total[b * rows : (b + 1) * rows].astype(BF16)


def shared_second_kernel(place, near, far, own, other, _, out):
    quarter = own.shape[1]
    rows = near.shape[0] // 2
    here = pl.multiple_of(place[0] * quarter, quarter)
    there = pl.multiple_of((1 - place[0]) * quarter, quarter)
    hidden = jax.nn.gelu(near[...].astype(F32) + far[...].astype(F32)).astype(BF16)
    left, right = dot(hidden, own[...]), dot(hidden, other[...])
    for b in range(2):
        turn = place[1] if b == 0 else 1 - place[1]
        at = pl.ds(pl.multiple_of(turn * rows, rows), rows)
        out[at, pl.ds(here, quarter)] = left[b * rows : (b + 1) * rows]
        out[at, pl.ds(there, quarter)] = right[b * rows : (b + 1) * rows]


def take_stage(place, source, own, after, grant):
    shape = (source.shape[0] // 2, *source.shape[1:])
    return pl.pallas_call(
        functools.partial(take_kernel, own),
        in_specs=[SMEM, HBM, ANY],
        out_specs=VMEM,
        out_shape=jax.ShapeDtypeStruct(shape, BF16),
        scratch_shapes=[pltpu.SemaphoreType.DMA(shape[:1])],
        compiler_params=granted(grant),
        cost_estimate=cost(KERNEL_FLOPS, 4 * shape[0] * shape[1] * shape[2]),
    )(place, source, after)


def kernel(body, after, shapes, place, *args):
    return pl.pallas_call(
        body,
        in_specs=[SMEM] + [VMEM] * len(args) + [ANY],
        out_specs=[VMEM] * len(shapes),
        out_shape=shapes,
        compiler_params=granted(),
        cost_estimate=cost(KERNEL_FLOPS, 1 << 20),
    )(place, *args, after)


def exchanged_partials(tokens, expert_ids, gate_weights, expert_in, expert_out, shared_in, shared_out):
    rows, width = tokens.shape
    half = width // 2
    picks = expert_ids.shape[1]
    group = expert_in.shape[0]
    local = group // 2
    hidden = expert_in.shape[2]
    groups = lax.axis_size(GROUP)
    spot = lax.axis_index(SIDE)
    side, core = spot // 2, spot % 2
    lead = lax.axis_index(GROUP) * group + core * local
    place = jnp.stack([core, side, lead]).astype(jnp.int32)

    def swap(value, axis, mask):
        return lax.ppermute(value, axis, [(i, i ^ mask) for i in range(lax.axis_size(axis))])

    def cross(value):
        return swap(value, SIDE, 2)

    def share(value):
        return swap(value, SIDE, 1)

    def take(source, own, after, grant):
        return take_stage(place, source, own, after, grant)

    give_in = take(expert_in, False, place, GIVE_GRANTS[0])
    other_in = share(give_in)
    block = jax.ShapeDtypeStruct((rows + META, half), BF16)
    mine, theirs = kernel(
        norm_kernel, give_in, [block] * 2,
        place, tokens, expert_ids.T, gate_weights.T,
    )
    peer = cross(theirs)
    own_in = take(expert_in, True, mine, GIVE_GRANTS[1])
    unit = jnp.concatenate([mine[:rows], peer[:rows], mine[rows:], peer[rows:]], axis=0)
    far = far_groups(groups)
    near = swap(unit, GROUP, 1)
    feeds = {"o": [unit], "n": [near], "l": [share(near)], "t": [share(unit)]}
    for g in far:
        if g % 2:
            got = swap(unit, GROUP, g)
        else:
            got = swap(feeds[str(g + 1)][0], GROUP, 1)
        feeds[str(g)] = [got, share(got)]

    firsts, kept, sums = {}, {}, []
    last, own_out = own_in, None

    def first(g):
        nonlocal last
        part, code, gate = first_stage(feeds[g], place, own_in, other_in, last, picks)
        firsts[g] = (part, code, gate, cross(part))
        last = code

    def second(g):
        nonlocal last, own_out
        part, code, gate, across = firsts[g]
        load = own_out is None
        keep, send = g not in "lt", g not in "on"
        outs = second_stage(
            len(feeds[g]), code, gate, part, across, place, expert_out if load else own_out,
            other_out, last, keep, send, load,
        )
        last = outs[0]
        own_out = outs[-1] if load else own_out
        if keep:
            kept[g] = outs[0]
        if not send:
            return
        came = share(outs[keep]).astype(F32)
        if g != "t":
            last = (kept.pop("n" if g == "l" else g) + came).astype(BF16)
            came = swap(last, GROUP, 1 if g == "l" else int(g)).astype(F32)
        sums.append(came)

    first("o")
    last = give_out = take(expert_out, False, last, GIVE_GRANTS[2])
    other_out = share(give_out)
    other_shared_in = share(shared_in)
    other_shared_out = share(shared_out)
    first("n")
    first("l")
    second("o")
    for g in far[:1]:
        first(str(g))
    second("n")
    second("l")
    for g in far[1:]:
        first(str(g))
    first("t")
    (shared_part,) = kernel(
        shared_first_kernel, last,
        [jax.ShapeDtypeStruct((2 * rows, hidden), BF16)],
        place, unit, shared_in, other_shared_in,
    )
    last = shared_part
    shared_far = cross(shared_part)
    for g in [*map(str, far), "t"]:
        second(g)
    (shared,) = kernel(
        shared_second_kernel, last,
        [jax.ShapeDtypeStruct((2 * rows, half), F32)],
        place, shared_part, shared_far, shared_out, other_shared_out,
    )

    total = sum(sums, shared + kept["o"])
    crossed = cross(total[rows:].astype(BF16)).astype(F32)
    stay = total[:rows]
    low = side == 0
    added = jnp.concatenate([jnp.where(low, stay, crossed), jnp.where(low, crossed, stay)], axis=1)
    return (tokens.astype(F32) + added).astype(BF16)


def exchange_fits(mesh, tokens, expert_ids, expert_in):
    groups, sides = mesh.shape[GROUP], mesh.shape[SIDE]
    blocks = mesh.shape[SWEEP] * groups
    rows, width = tokens.shape[0] // (blocks * sides), tokens.shape[1]
    return (
        sides == 4
        and expert_in.shape[0] % (blocks * 16) == 0
        and groups in (2, 4, 8)
        and rows % 128 == 0
        and width % 512 == 0
        and width // 2 >= 3 * rows
        and expert_ids.shape[1] <= 8
        and expert_in.shape[2] % 128 == 0
    )


def far_groups(groups):
    return list(range(groups - 1, 1, -1))


def solution(mesh):
    rows = P((SWEEP, GROUP, SIDE), None)
    placed = (
        rows,
        rows,
        rows,
        P((SWEEP, GROUP), SIDE, None),
        P((SWEEP, GROUP), None, SIDE),
        P((SWEEP, SIDE), None),
        P(SWEEP, SIDE),
    )
    spread = functools.partial(
        jax.shard_map, mesh=mesh, in_specs=placed, out_specs=rows, check_vma=False
    )

    def program(*args):
        if not exchange_fits(mesh, args[0], args[1], args[3]):
            return spread(gathered_weights)(*args)
        step = spread(exchanged_partials)
        return step(*args)

    return program
```

```python
import functools

import jax
import jax.numpy as jnp
from jax import lax
from jax.experimental import pallas as pl
from jax.experimental.pallas import tpu as pltpu
from jax.sharding import PartitionSpec as P


CAP = 20
SWEEP, GROUP, SIDE = "sweep", "expert", "dp"
F32 = jnp.float32
BF16 = jnp.bfloat16
KERNEL_FLOPS = 10_000_000
META = 8


def layer_norm(tokens):
    values = tokens.astype(F32)
    center = values - jnp.mean(values, axis=-1, keepdims=True)
    spread = jnp.mean(center * center, axis=-1, keepdims=True)
    return (center * lax.rsqrt(spread + 1e-06)).astype(BF16)


def copy_slots(expert_ids, expert_count):
    expert_iota = jnp.arange(expert_count, dtype=jnp.int32)
    matches = (expert_ids[..., None] == expert_iota).astype(jnp.int32)
    per_token = jnp.sum(matches, axis=-2, dtype=jnp.int32)
    earlier = jnp.cumsum(per_token, axis=-2, dtype=jnp.int32) - per_token
    return jnp.sum(matches * earlier[..., None, :], axis=-1, dtype=jnp.int32)


def run_experts(shard_piece, weight_in, weight_out):
    pre_act = jnp.einsum("gesd,edf->gesf", shard_piece, weight_in, preferred_element_type=F32)
    hidden = jax.nn.gelu(pre_act).astype(BF16)
    return jnp.einsum("gesf,efd->gesd", hidden, weight_out, preferred_element_type=F32).astype(BF16)


def gathered_weights(tokens, expert_ids, gate_weights, expert_in, expert_out, shared_in, shared_out):
    row_count, model_width = tokens.shape
    pick_count = expert_ids.shape[1]
    local_count = expert_in.shape[0]
    group_count = lax.axis_size(GROUP)
    expert_total = local_count * group_count
    normed = layer_norm(tokens)
    full_in = lax.all_gather(expert_in, SIDE, axis=1, tiled=True)
    full_out = lax.all_gather(expert_out, SIDE, axis=2, tiled=True)
    slot_of = copy_slots(expert_ids, expert_total)
    positions = (expert_ids * CAP + slot_of).reshape(-1)
    copies = jnp.repeat(normed, pick_count, axis=0)
    outgoing = jnp.zeros((expert_total * CAP, model_width), BF16).at[positions].set(copies)
    outgoing = outgoing.reshape(group_count, local_count, CAP, model_width)
    received = lax.all_to_all(outgoing, GROUP, split_axis=0, concat_axis=0, tiled=True)
    returned = lax.all_to_all(
        run_experts(received, full_in, full_out), GROUP, split_axis=0, concat_axis=0, tiled=True
    )
    results = returned.reshape(expert_total * CAP, model_width)[positions].reshape(
        row_count, pick_count, model_width
    )
    routed = jnp.sum(results.astype(F32) * gate_weights[:, :, None], axis=1)
    shared_pre = jnp.dot(
        normed, lax.all_gather(shared_in, SIDE, axis=0, tiled=True), preferred_element_type=F32
    )
    shared_hidden = jax.nn.gelu(shared_pre).astype(BF16)
    shared_result = jnp.dot(
        shared_hidden,
        lax.all_gather(shared_out, SIDE, axis=1, tiled=True),
        preferred_element_type=F32,
    )
    return (tokens.astype(F32) + shared_result + routed).astype(BF16)


def dot(a, b):
    return jnp.dot(a, b, preferred_element_type=F32)


def cost(flops, moved):
    return pl.CostEstimate(flops=int(flops), bytes_accessed=int(moved), transcendentals=0)


def half_copies(source, held, base, came):
    return [
        pltpu.make_async_copy(source.at[base + e], held.at[e], came.at[e])
        for e in range(held.shape[0])
    ]


def norm_kernel(place, tokens, ids, gates, _, mine, theirs):
    rows, width = tokens.shape
    half = width // 2
    values = tokens[...].astype(F32)
    center = values - jnp.mean(values, axis=-1, keepdims=True)
    spread = jnp.mean(center * center, axis=-1, keepdims=True)
    normed = (center * lax.rsqrt(spread + 1e-06)).astype(BF16)
    low = place[1] == 0
    mine[0:rows, :] = jnp.where(low, normed[:, :half], normed[:, half:])
    theirs[0:rows, :] = jnp.where(low, normed[:, half:], normed[:, :half])
    gate = gates[...]
    high = gate.astype(BF16).astype(F32)
    rest = gate - high
    picks = ids.shape[0]
    spare = jnp.zeros((picks, half - 3 * rows), F32)
    table = jnp.concatenate([ids[...].astype(F32), high, rest, spare], axis=1)
    if picks < META:
        table = jnp.concatenate([table, jnp.zeros((META - picks, half), F32)], axis=0)
    table = table.astype(BF16)
    mine[rows : rows + META, :] = table
    theirs[rows : rows + META, :] = table


def take_kernel(own, place, source, after, taken, came):
    local = taken.shape[0]
    copies = half_copies(source, taken, (place[0] if own else 1 - place[0]) * local, came)
    for c in copies:
        c.start()
    for c in copies:
        c.wait()


def selection(codes, rows):
    count, tokens = codes.shape
    wanted = lax.broadcasted_iota(jnp.int32, (rows, tokens), 0).astype(F32)
    return [(wanted == codes[e : e + 1, :]).astype(F32) for e in range(count)]


def first_kernel(units, picks, place, *refs):
    feeds, refs = refs[:units], refs[units:]
    own, other, _, part, code, gate, packed = refs
    local, rows, half = packed.shape
    slots = rows // (2 * units)
    tokens = feeds[0].shape[0] // 2 - META
    before = (
        lax.broadcasted_iota(jnp.int32, (tokens, tokens), 0)
        < lax.broadcasted_iota(jnp.int32, (tokens, tokens), 1)
    ).astype(F32).astype(BF16)
    expert = (lax.broadcasted_iota(jnp.int32, (local, tokens), 0) + place[2]).astype(F32)
    for u in range(units):
        for b in range(2):
            at = 2 * tokens + b * META
            table = feeds[u][at : at + META, 0 : 3 * tokens].astype(F32)
            named = jnp.zeros((local, tokens), F32)
            weight = jnp.zeros((local, tokens), F32)
            for k in range(picks):
                same = table[k : k + 1, 0:tokens] == expert
                value = table[k : k + 1, tokens : 2 * tokens] + table[k : k + 1, 2 * tokens :]
                named = jnp.where(same, 1.0, named)
                weight = jnp.where(same, value, weight)
            rank = dot(named.astype(BF16), before)
            turn = place[1] if b == 0 else 1 - place[1]
            base = ((2 * u + turn) * slots).astype(F32)
            column = (2 * u + b) * tokens
            code[:, column : column + tokens] = jnp.where(named > 0, rank + base, -1.0)
            gate[:, column : column + tokens] = weight
    pick = jnp.concatenate(selection(code[...], rows), axis=0).astype(BF16)
    wide = half // 3 if half % 384 == 0 else half
    for n in range(half // wide):
        columns = slice(n * wide, (n + 1) * wide)
        chosen = sum(
            dot(pick[:, 2 * u * tokens : 2 * (u + 1) * tokens], feeds[u][0 : 2 * tokens, columns])
            for u in range(units)
        )
        for e in range(local):
            packed[e, :, columns] = chosen[e * rows : (e + 1) * rows].astype(BF16)

    quarter = half // 2
    here = pl.multiple_of(place[0] * quarter, quarter)
    there = pl.multiple_of((1 - place[0]) * quarter, quarter)

    @pl.loop(0, local // 2)
    def _(pair):
        for e in (2 * pair, 2 * pair + 1):
            total = dot(packed[e, :, pl.ds(here, quarter)], own[e])
            total += dot(packed[e, :, pl.ds(there, quarter)], other[e])
            part[e] = total.astype(BF16)


def second_kernel(units, keep, send, join, load, place, *refs):
    code, gate, near, far, source, other, after = refs[:7]
    shown = keep + send + join
    outs, refs = refs[7 : 7 + shown], refs[7 + shown :]
    own, (total, *came) = (refs[0], refs[1:]) if load else (source, refs)
    local = code.shape[0]
    rows = near.shape[1]
    half = total.shape[1]
    if load:
        for c in half_copies(source, own, place[0] * local, came[0]):
            c.start()
    quarter = half // 2
    here = pl.multiple_of(place[0] * quarter, quarter)
    there = pl.multiple_of((1 - place[0]) * quarter, quarter)
    wanted = lax.broadcasted_iota(jnp.int32, (rows, code.shape[1]), 0).astype(F32)

    @pl.loop(0, local // 2)
    def _(pair):
        for e in (2 * pair, 2 * pair + 1):
            same = wanted == code[pl.ds(e, 1), :]
            scale = jnp.sum(jnp.where(same, gate[pl.ds(e, 1), :], 0.0), axis=1, keepdims=True)
            hidden = jax.nn.gelu(near[e].astype(F32) + far[e].astype(F32)).astype(BF16)
            at = pl.ds(pl.multiple_of(e * rows, rows), rows)
            total[at, pl.ds(there, quarter)] = dot(hidden, other[e]) * scale
            if load:
                base = place[0] * local
                pltpu.make_async_copy(source.at[base + e], own.at[e], came[0].at[e]).wait()
            total[at, pl.ds(here, quarter)] = dot(hidden, own[e]) * scale

    pick = jnp.concatenate(selection(code[...], rows), axis=0).astype(BF16)
    wide = half // 3 if half % 384 == 0 else half
    count = code.shape[1] // units
    for n in range(half // wide):
        columns = slice(n * wide, (n + 1) * wide)
        summed = lax.dot_general(
            pick,
            total[:, columns].astype(BF16),
            (((0,), (0,)), ((), ())),
            preferred_element_type=F32,
        )
        slot = 0
        if keep:
            outs[slot][:, columns] = summed[0:count]
            slot += 1
        if send:
            outs[slot][:, columns] = summed[(units - 1) * count :].astype(BF16)
        if join:
            outs[slot][:, columns] = (summed + after[:, columns].astype(F32)).astype(BF16)


SMEM = pl.BlockSpec(memory_space=pltpu.SMEM)
VMEM = pl.BlockSpec(memory_space=pltpu.VMEM)
ANY = pl.BlockSpec(memory_space=pl.ANY)
HBM = pl.BlockSpec(memory_space=pltpu.HBM)
GRANT = 24 << 20
GIVE_GRANTS = (46 << 20, 42 << 20, 42 << 20)
SECOND_GRANT = 36 << 20


def granted(size=GRANT):
    return pltpu.CompilerParams(vmem_limit_bytes=size)


def first_stage(feeds, place, own, other, after, picks):
    units = len(feeds)
    local, quarter, hidden = other.shape
    half = 2 * quarter
    tokens = feeds[0].shape[0] // 2 - META
    rows = 2 * units * CAP
    table = jax.ShapeDtypeStruct((local, 2 * units * tokens), F32)
    return pl.pallas_call(
        functools.partial(first_kernel, units, picks),
        in_specs=[SMEM] + [VMEM] * (units + 2) + [ANY],
        out_specs=[VMEM] * 3,
        scratch_shapes=[pltpu.VMEM((local, rows, half), BF16)],
        out_shape=[jax.ShapeDtypeStruct((local, rows, hidden), BF16), table, table],
        compiler_params=granted(),
        cost_estimate=cost(KERNEL_FLOPS, 2 * local * half * hidden),
    )(place, *feeds, own, other, after)


def second_stage(units, code, gate, near, far, place, own, other, after, keep, send, join, load):
    local, hidden, quarter = other.shape
    half = 2 * quarter
    rows = near.shape[1]
    count = code.shape[1] // units
    shapes = []
    if keep:
        shapes.append(jax.ShapeDtypeStruct((count, half), F32))
    if send or join:
        shapes.append(jax.ShapeDtypeStruct((count, half), BF16))
    if load:
        shapes.append(jax.ShapeDtypeStruct(other.shape, BF16))
    return pl.pallas_call(
        functools.partial(second_kernel, units, keep, send, join, load),
        in_specs=[SMEM] + [VMEM] * 4 + [HBM if load else VMEM, VMEM, VMEM if join else ANY],
        out_specs=[VMEM] * len(shapes),
        scratch_shapes=[pltpu.VMEM((local * rows, half), F32)]
        + [pltpu.SemaphoreType.DMA((local,))] * load,
        out_shape=shapes,
        compiler_params=granted(SECOND_GRANT if load else GRANT),
        cost_estimate=cost(KERNEL_FLOPS, 2 * local * half * hidden),
    )(place, code, gate, near, far, own, other, after)


def shared_first_kernel(place, feed, own, other, _, part):
    quarter = own.shape[0]
    rows = part.shape[0] // 2
    here = pl.multiple_of(place[0] * quarter, quarter)
    there = pl.multiple_of((1 - place[0]) * quarter, quarter)
    total = dot(feed[0 : 2 * rows, pl.ds(here, quarter)], own[...])
    total += dot(feed[0 : 2 * rows, pl.ds(there, quarter)], other[...])
    for b in range(2):
        turn = place[1] if b == 0 else 1 - place[1]
        at = pl.ds(pl.multiple_of(turn * rows, rows), rows)
        part[at, :] = total[b * rows : (b + 1) * rows].astype(BF16)


def shared_second_kernel(place, near, far, own, other, _, out):
    quarter = own.shape[1]
    rows = near.shape[0] // 2
    here = pl.multiple_of(place[0] * quarter, quarter)
    there = pl.multiple_of((1 - place[0]) * quarter, quarter)
    hidden = jax.nn.gelu(near[...].astype(F32) + far[...].astype(F32)).astype(BF16)
    left, right = dot(hidden, own[...]), dot(hidden, other[...])
    for b in range(2):
        turn = place[1] if b == 0 else 1 - place[1]
        at = pl.ds(pl.multiple_of(turn * rows, rows), rows)
        out[at, pl.ds(here, quarter)] = left[b * rows : (b + 1) * rows]
        out[at, pl.ds(there, quarter)] = right[b * rows : (b + 1) * rows]


def take_stage(place, source, own, after, grant):
    shape = (source.shape[0] // 2, *source.shape[1:])
    return pl.pallas_call(
        functools.partial(take_kernel, own),
        in_specs=[SMEM, HBM, ANY],
        out_specs=VMEM,
        out_shape=jax.ShapeDtypeStruct(shape, BF16),
        scratch_shapes=[pltpu.SemaphoreType.DMA(shape[:1])],
        compiler_params=granted(grant),
        cost_estimate=cost(KERNEL_FLOPS, 4 * shape[0] * shape[1] * shape[2]),
    )(place, source, after)


def kernel(body, after, shapes, place, *args):
    return pl.pallas_call(
        body,
        in_specs=[SMEM] + [VMEM] * len(args) + [ANY],
        out_specs=[VMEM] * len(shapes),
        out_shape=shapes,
        compiler_params=granted(),
        cost_estimate=cost(KERNEL_FLOPS, 1 << 20),
    )(place, *args, after)


def exchanged_partials(tokens, expert_ids, gate_weights, expert_in, expert_out, shared_in, shared_out):
    rows, width = tokens.shape
    half = width // 2
    picks = expert_ids.shape[1]
    group = expert_in.shape[0]
    local = group // 2
    hidden = expert_in.shape[2]
    groups = lax.axis_size(GROUP)
    spot = lax.axis_index(SIDE)
    side, core = spot // 2, spot % 2
    lead = lax.axis_index(GROUP) * group + core * local
    place = jnp.stack([core, side, lead]).astype(jnp.int32)

    def swap(value, axis, mask):
        return lax.ppermute(value, axis, [(i, i ^ mask) for i in range(lax.axis_size(axis))])

    def cross(value):
        return swap(value, SIDE, 2)

    def share(value):
        return swap(value, SIDE, 1)

    def take(source, own, after, grant):
        return take_stage(place, source, own, after, grant)

    give_in = take(expert_in, False, place, GIVE_GRANTS[0])
    other_in = share(give_in)
    block = jax.ShapeDtypeStruct((rows + META, half), BF16)
    mine, theirs = kernel(
        norm_kernel, give_in, [block] * 2,
        place, tokens, expert_ids.T, gate_weights.T,
    )
    peer = cross(theirs)
    own_in = take(expert_in, True, mine, GIVE_GRANTS[1])
    far = far_groups(groups)
    unit = pair_up(mine, peer, rows)
    near = pair_up(swap(mine, GROUP, 1), swap(peer, GROUP, 1), rows)
    feeds = {"o": [unit], "n": [near], "l": [share(near)], "t": [share(unit)]}
    for g in far:
        if g % 2:
            early = swap(mine, GROUP, g)
            got = pair_up(early, swap(peer, GROUP, g), rows)
        else:
            got = swap(feeds[str(g + 1)][0], GROUP, 1)
        feeds[str(g)] = [got, share(got)]
    if far:
        feeds["m"] = [feeds["2"].pop()]

    firsts, kept, sums = {}, {}, []
    last, own_out = own_in, None

    def first(g):
        nonlocal last
        part, code, gate = first_stage(feeds[g], place, own_in, other_in, last, picks)
        firsts[g] = (part, code, gate, cross(part))
        last = code

    def second(g):
        nonlocal last, own_out
        part, code, gate, across = firsts[g]
        load = own_out is None
        keep, send, join = g not in "ltm2", g not in "on2", g == "2"
        outs = second_stage(
            len(feeds[g]), code, gate, part, across, place, expert_out if load else own_out,
            other_out, kept["m"] if join else last, keep, send, join, load,
        )
        last = outs[0]
        own_out = outs[-1] if load else own_out
        if keep:
            kept[g] = outs[0]
        if join:
            sums.append(swap(last, GROUP, 2).astype(F32))
        if not send:
            return
        came = share(outs[keep])
        if g == "m":
            kept[g] = came
            return
        came = came.astype(F32)
        if g != "t":
            last = (kept.pop("n" if g == "l" else g) + came).astype(BF16)
            came = swap(last, GROUP, 1 if g == "l" else int(g)).astype(F32)
        sums.append(came)

    first("o")
    last = give_out = take(expert_out, False, last, GIVE_GRANTS[2])
    other_out = share(give_out)
    other_shared_in = share(shared_in)
    other_shared_out = share(shared_out)
    tail = [str(g) for g in far[:-1]] + ["m", "2"] * bool(far)
    first("n")
    first("l")
    second("o")
    for g in tail[:1]:
        first(g)
    second("n")
    second("l")
    for g in tail[1:]:
        first(g)
    first("t")
    (shared_part,) = kernel(
        shared_first_kernel, last,
        [jax.ShapeDtypeStruct((2 * rows, hidden), BF16)],
        place, unit, shared_in, other_shared_in,
    )
    last = shared_part
    shared_far = cross(shared_part)
    for g in [*tail, "t"]:
        second(g)
    (shared,) = kernel(
        shared_second_kernel, last,
        [jax.ShapeDtypeStruct((2 * rows, half), F32)],
        place, shared_part, shared_far, shared_out, other_shared_out,
    )

    total = sum(sums, shared + kept["o"])
    crossed = cross(total[rows:].astype(BF16)).astype(F32)
    stay = total[:rows]
    low = side == 0
    added = jnp.concatenate([jnp.where(low, stay, crossed), jnp.where(low, crossed, stay)], axis=1)
    return (tokens.astype(F32) + added).astype(BF16)


def exchange_fits(mesh, tokens, expert_ids, expert_in):
    groups, sides = mesh.shape[GROUP], mesh.shape[SIDE]
    blocks = mesh.shape[SWEEP] * groups
    rows, width = tokens.shape[0] // (blocks * sides), tokens.shape[1]
    return (
        sides == 4
        and expert_in.shape[0] % (blocks * 16) == 0
        and groups in (4, 8)
        and rows % 128 == 0
        and width % 512 == 0
        and width // 2 >= 3 * rows
        and expert_ids.shape[1] <= META
        and expert_in.shape[2] % 128 == 0
    )


def pair_up(first, second, rows):
    return jnp.concatenate([first[:rows], second[:rows], first[rows:], second[rows:]], axis=0)


def far_groups(groups):
    return list(range(groups - 1, 1, -1))


def solution(mesh):
    rows = P((SWEEP, GROUP, SIDE), None)
    placed = (
        rows,
        rows,
        rows,
        P((SWEEP, GROUP), SIDE, None),
        P((SWEEP, GROUP), None, SIDE),
        P((SWEEP, SIDE), None),
        P(SWEEP, SIDE),
    )
    spread = functools.partial(
        jax.shard_map, mesh=mesh, in_specs=placed, out_specs=rows, check_vma=False
    )

    def program(*args):
        if not exchange_fits(mesh, args[0], args[1], args[3]):
            return spread(gathered_weights)(*args)
        step = spread(exchanged_partials)
        return step(*args)

    return program
```

```python
import functools

import jax
import jax.numpy as jnp
from jax import lax
from jax.experimental import pallas as pl
from jax.experimental.pallas import tpu as pltpu
from jax.sharding import PartitionSpec as P


CAP = 20
SWEEP, GROUP, SIDE = "sweep", "expert", "dp"
F32 = jnp.float32
BF16 = jnp.bfloat16
KERNEL_FLOPS = 10_000_000
META = 8


def layer_norm(tokens):
    values = tokens.astype(F32)
    center = values - jnp.mean(values, axis=-1, keepdims=True)
    spread = jnp.mean(center * center, axis=-1, keepdims=True)
    return (center * lax.rsqrt(spread + 1e-06)).astype(BF16)


def copy_slots(expert_ids, expert_count):
    expert_iota = jnp.arange(expert_count, dtype=jnp.int32)
    matches = (expert_ids[..., None] == expert_iota).astype(jnp.int32)
    per_token = jnp.sum(matches, axis=-2, dtype=jnp.int32)
    earlier = jnp.cumsum(per_token, axis=-2, dtype=jnp.int32) - per_token
    return jnp.sum(matches * earlier[..., None, :], axis=-1, dtype=jnp.int32)


def run_experts(shard_piece, weight_in, weight_out):
    pre_act = jnp.einsum("gesd,edf->gesf", shard_piece, weight_in, preferred_element_type=F32)
    hidden = jax.nn.gelu(pre_act).astype(BF16)
    return jnp.einsum("gesf,efd->gesd", hidden, weight_out, preferred_element_type=F32).astype(BF16)


def gathered_weights(tokens, expert_ids, gate_weights, expert_in, expert_out, shared_in, shared_out):
    row_count, model_width = tokens.shape
    pick_count = expert_ids.shape[1]
    local_count = expert_in.shape[0]
    group_count = lax.axis_size(GROUP)
    expert_total = local_count * group_count
    normed = layer_norm(tokens)
    full_in = lax.all_gather(expert_in, SIDE, axis=1, tiled=True)
    full_out = lax.all_gather(expert_out, SIDE, axis=2, tiled=True)
    slot_of = copy_slots(expert_ids, expert_total)
    positions = (expert_ids * CAP + slot_of).reshape(-1)
    copies = jnp.repeat(normed, pick_count, axis=0)
    outgoing = jnp.zeros((expert_total * CAP, model_width), BF16).at[positions].set(copies)
    outgoing = outgoing.reshape(group_count, local_count, CAP, model_width)
    received = lax.all_to_all(outgoing, GROUP, split_axis=0, concat_axis=0, tiled=True)
    returned = lax.all_to_all(
        run_experts(received, full_in, full_out), GROUP, split_axis=0, concat_axis=0, tiled=True
    )
    results = returned.reshape(expert_total * CAP, model_width)[positions].reshape(
        row_count, pick_count, model_width
    )
    routed = jnp.sum(results.astype(F32) * gate_weights[:, :, None], axis=1)
    shared_pre = jnp.dot(
        normed, lax.all_gather(shared_in, SIDE, axis=0, tiled=True), preferred_element_type=F32
    )
    shared_hidden = jax.nn.gelu(shared_pre).astype(BF16)
    shared_result = jnp.dot(
        shared_hidden,
        lax.all_gather(shared_out, SIDE, axis=1, tiled=True),
        preferred_element_type=F32,
    )
    return (tokens.astype(F32) + shared_result + routed).astype(BF16)


def dot(a, b):
    return jnp.dot(a, b, preferred_element_type=F32)


def cost(flops, moved):
    return pl.CostEstimate(flops=int(flops), bytes_accessed=int(moved), transcendentals=0)


def half_copies(source, held, base, came):
    return [
        pltpu.make_async_copy(source.at[base + e], held.at[e], came.at[e])
        for e in range(held.shape[0])
    ]


def norm_kernel(place, tokens, ids, gates, _, mine, theirs):
    rows, width = tokens.shape
    half = width // 2
    values = tokens[...].astype(F32)
    center = values - jnp.mean(values, axis=-1, keepdims=True)
    spread = jnp.mean(center * center, axis=-1, keepdims=True)
    normed = (center * lax.rsqrt(spread + 1e-06)).astype(BF16)
    low = place[1] == 0
    mine[0:rows, :] = jnp.where(low, normed[:, :half], normed[:, half:])
    theirs[0:rows, :] = jnp.where(low, normed[:, half:], normed[:, :half])
    gate = gates[...]
    high = gate.astype(BF16).astype(F32)
    rest = gate - high
    picks = ids.shape[0]
    spare = jnp.zeros((picks, half - 3 * rows), F32)
    table = jnp.concatenate([ids[...].astype(F32), high, rest, spare], axis=1)
    if picks < META:
        table = jnp.concatenate([table, jnp.zeros((META - picks, half), F32)], axis=0)
    table = table.astype(BF16)
    mine[rows : rows + META, :] = table
    theirs[rows : rows + META, :] = table


def take_kernel(own, place, source, after, taken, came):
    local = taken.shape[0]
    copies = half_copies(source, taken, (place[0] if own else 1 - place[0]) * local, came)
    for c in copies:
        c.start()
    for c in copies:
        c.wait()


def selection(codes, rows):
    count, tokens = codes.shape
    wanted = lax.broadcasted_iota(jnp.int32, (rows, tokens), 0).astype(F32)
    return [(wanted == codes[e : e + 1, :]).astype(F32) for e in range(count)]


def first_kernel(feed_count, tokens, picks, place, *refs):
    feeds, refs = refs[:feed_count], refs[feed_count:]
    own, other, _, part, code, gate, *pair, packed = refs
    local, rows, half = packed.shape
    block_counts = [feed.shape[0] // (tokens + META) for feed in feeds]
    for unit in pair:
        for b, feed in enumerate(feeds):
            at = len(feeds) * tokens + b * META
            unit[b * tokens : (b + 1) * tokens, :] = feed[0:tokens, :]
            unit[at : at + META, :] = feed[tokens:, :]
    slots = rows // sum(block_counts)
    before = (
        lax.broadcasted_iota(jnp.int32, (tokens, tokens), 0)
        < lax.broadcasted_iota(jnp.int32, (tokens, tokens), 1)
    ).astype(F32).astype(BF16)
    expert = (lax.broadcasted_iota(jnp.int32, (local, tokens), 0) + place[2]).astype(F32)
    tables = [
        feed[count * tokens + b * META : count * tokens + (b + 1) * META, 0 : 3 * tokens]
        for feed, count in zip(feeds, block_counts)
        for b in range(count)
    ]
    for i, table in enumerate(tables):
        table = table.astype(F32)
        named = jnp.zeros((local, tokens), F32)
        weight = jnp.zeros((local, tokens), F32)
        for k in range(picks):
            same = table[k : k + 1, 0:tokens] == expert
            value = table[k : k + 1, tokens : 2 * tokens] + table[k : k + 1, 2 * tokens :]
            named = jnp.where(same, 1.0, named)
            weight = jnp.where(same, value, weight)
        rank = dot(named.astype(BF16), before)
        turn = 1 - place[1] if i % 2 else place[1]
        base = ((i - i % 2 + turn) * slots).astype(F32)
        column = i * tokens
        code[:, column : column + tokens] = jnp.where(named > 0, rank + base, -1.0)
        gate[:, column : column + tokens] = weight
    pick = jnp.concatenate(selection(code[...], rows), axis=0).astype(BF16)
    wide = half // 3 if half % 384 == 0 else half
    for n in range(half // wide):
        columns = slice(n * wide, (n + 1) * wide)
        chosen, column = 0.0, 0
        for feed, count in zip(feeds, block_counts):
            held = slice(column, column + count * tokens)
            chosen += dot(pick[:, held], feed[0 : count * tokens, columns])
            column += count * tokens
        for e in range(local):
            packed[e, :, columns] = chosen[e * rows : (e + 1) * rows].astype(BF16)

    quarter = half // 2
    here = pl.multiple_of(place[0] * quarter, quarter)
    there = pl.multiple_of((1 - place[0]) * quarter, quarter)

    @pl.loop(0, local // 2)
    def _(pair):
        for e in (2 * pair, 2 * pair + 1):
            total = dot(packed[e, :, pl.ds(here, quarter)], own[e])
            total += dot(packed[e, :, pl.ds(there, quarter)], other[e])
            part[e] = total.astype(BF16)


def second_kernel(units, keep, send, join, load, place, *refs):
    code, gate, near, far, source, other, after = refs[:7]
    shown = keep + send + join
    outs, refs = refs[7 : 7 + shown], refs[7 + shown :]
    own, (total, *came) = (refs[0], refs[1:]) if load else (source, refs)
    local = code.shape[0]
    rows = near.shape[1]
    half = total.shape[1]
    if load:
        for c in half_copies(source, own, place[0] * local, came[0]):
            c.start()
    quarter = half // 2
    here = pl.multiple_of(place[0] * quarter, quarter)
    there = pl.multiple_of((1 - place[0]) * quarter, quarter)
    wanted = lax.broadcasted_iota(jnp.int32, (rows, code.shape[1]), 0).astype(F32)

    @pl.loop(0, local // 2)
    def _(pair):
        for e in (2 * pair, 2 * pair + 1):
            same = wanted == code[pl.ds(e, 1), :]
            scale = jnp.sum(jnp.where(same, gate[pl.ds(e, 1), :], 0.0), axis=1, keepdims=True)
            hidden = jax.nn.gelu(near[e].astype(F32) + far[e].astype(F32)).astype(BF16)
            at = pl.ds(pl.multiple_of(e * rows, rows), rows)
            total[at, pl.ds(there, quarter)] = dot(hidden, other[e]) * scale
            if load:
                base = place[0] * local
                pltpu.make_async_copy(source.at[base + e], own.at[e], came[0].at[e]).wait()
            total[at, pl.ds(here, quarter)] = dot(hidden, own[e]) * scale

    pick = jnp.concatenate(selection(code[...], rows), axis=0).astype(BF16)
    wide = half // 3 if half % 384 == 0 else half
    count = code.shape[1] // units
    for n in range(half // wide):
        columns = slice(n * wide, (n + 1) * wide)
        summed = lax.dot_general(
            pick,
            total[:, columns].astype(BF16),
            (((0,), (0,)), ((), ())),
            preferred_element_type=F32,
        )
        slot = 0
        if keep:
            outs[slot][:, columns] = summed[0:count]
            slot += 1
        if send:
            outs[slot][:, columns] = summed[(units - 1) * count :].astype(BF16)
        if join:
            outs[slot][:, columns] = (summed + after[:, columns].astype(F32)).astype(BF16)


SMEM = pl.BlockSpec(memory_space=pltpu.SMEM)
VMEM = pl.BlockSpec(memory_space=pltpu.VMEM)
ANY = pl.BlockSpec(memory_space=pl.ANY)
HBM = pl.BlockSpec(memory_space=pltpu.HBM)
GRANT = 24 << 20
GIVE_GRANTS = (46 << 20, 42 << 20, 42 << 20)
SECOND_GRANT = 35 << 20


def granted(size=GRANT):
    return pltpu.CompilerParams(vmem_limit_bytes=size)


def first_stage(feeds, tokens, place, own, other, after, picks):
    local, quarter, hidden = other.shape
    half = 2 * quarter
    blocks = sum(feed.shape[0] for feed in feeds) // (tokens + META)
    rows = blocks * CAP
    pair = [jax.ShapeDtypeStruct((blocks * (tokens + META), half), BF16)] * (len(feeds) == blocks)
    table = jax.ShapeDtypeStruct((local, blocks * tokens), F32)
    return pl.pallas_call(
        functools.partial(first_kernel, len(feeds), tokens, picks),
        in_specs=[SMEM] + [VMEM] * (len(feeds) + 2) + [ANY],
        out_specs=[VMEM] * (3 + len(pair)),
        scratch_shapes=[pltpu.VMEM((local, rows, half), BF16)],
        out_shape=[jax.ShapeDtypeStruct((local, rows, hidden), BF16), table, table, *pair],
        compiler_params=granted(),
        cost_estimate=cost(KERNEL_FLOPS, 2 * local * half * hidden),
    )(place, *feeds, own, other, after)


def second_stage(units, code, gate, near, far, place, own, other, after, keep, send, join, load):
    local, hidden, quarter = other.shape
    half = 2 * quarter
    rows = near.shape[1]
    count = code.shape[1] // units
    shapes = []
    if keep:
        shapes.append(jax.ShapeDtypeStruct((count, half), F32))
    if send or join:
        shapes.append(jax.ShapeDtypeStruct((count, half), BF16))
    if load:
        shapes.append(jax.ShapeDtypeStruct(other.shape, BF16))
    return pl.pallas_call(
        functools.partial(second_kernel, units, keep, send, join, load),
        in_specs=[SMEM] + [VMEM] * 4 + [HBM if load else VMEM, VMEM, VMEM if join else ANY],
        out_specs=[VMEM] * len(shapes),
        scratch_shapes=[pltpu.VMEM((local * rows, half), F32)]
        + [pltpu.SemaphoreType.DMA((local,))] * load,
        out_shape=shapes,
        compiler_params=granted(SECOND_GRANT if load else GRANT),
        cost_estimate=cost(KERNEL_FLOPS, 2 * local * half * hidden),
    )(place, code, gate, near, far, own, other, after)


def shared_first_kernel(place, feed, own, other, _, part):
    quarter = own.shape[0]
    rows = part.shape[0] // 2
    here = pl.multiple_of(place[0] * quarter, quarter)
    there = pl.multiple_of((1 - place[0]) * quarter, quarter)
    total = dot(feed[0 : 2 * rows, pl.ds(here, quarter)], own[...])
    total += dot(feed[0 : 2 * rows, pl.ds(there, quarter)], other[...])
    for b in range(2):
        turn = place[1] if b == 0 else 1 - place[1]
        at = pl.ds(pl.multiple_of(turn * rows, rows), rows)
        part[at, :] = total[b * rows : (b + 1) * rows].astype(BF16)


def shared_second_kernel(place, near, far, own, other, _, out):
    quarter = own.shape[1]
    rows = near.shape[0] // 2
    here = pl.multiple_of(place[0] * quarter, quarter)
    there = pl.multiple_of((1 - place[0]) * quarter, quarter)
    hidden = jax.nn.gelu(near[...].astype(F32) + far[...].astype(F32)).astype(BF16)
    left, right = dot(hidden, own[...]), dot(hidden, other[...])
    for b in range(2):
        turn = place[1] if b == 0 else 1 - place[1]
        at = pl.ds(pl.multiple_of(turn * rows, rows), rows)
        out[at, pl.ds(here, quarter)] = left[b * rows : (b + 1) * rows]
        out[at, pl.ds(there, quarter)] = right[b * rows : (b + 1) * rows]


def take_stage(place, source, own, after, grant):
    shape = (source.shape[0] // 2, *source.shape[1:])
    return pl.pallas_call(
        functools.partial(take_kernel, own),
        in_specs=[SMEM, HBM, ANY],
        out_specs=VMEM,
        out_shape=jax.ShapeDtypeStruct(shape, BF16),
        scratch_shapes=[pltpu.SemaphoreType.DMA(shape[:1])],
        compiler_params=granted(grant),
        cost_estimate=cost(KERNEL_FLOPS, 4 * shape[0] * shape[1] * shape[2]),
    )(place, source, after)


def kernel(body, after, shapes, place, *args):
    return pl.pallas_call(
        body,
        in_specs=[SMEM] + [VMEM] * len(args) + [ANY],
        out_specs=[VMEM] * len(shapes),
        out_shape=shapes,
        compiler_params=granted(),
        cost_estimate=cost(KERNEL_FLOPS, 1 << 20),
    )(place, *args, after)


def exchanged_partials(tokens, expert_ids, gate_weights, expert_in, expert_out, shared_in, shared_out):
    rows, width = tokens.shape
    half = width // 2
    picks = expert_ids.shape[1]
    group = expert_in.shape[0]
    local = group // 2
    hidden = expert_in.shape[2]
    groups = lax.axis_size(GROUP)
    spot = lax.axis_index(SIDE)
    side, core = spot // 2, spot % 2
    lead = lax.axis_index(GROUP) * group + core * local
    place = jnp.stack([core, side, lead]).astype(jnp.int32)

    def swap(value, axis, mask):
        return lax.ppermute(value, axis, [(i, i ^ mask) for i in range(lax.axis_size(axis))])

    def cross(value):
        return swap(value, SIDE, 2)

    def share(value):
        return swap(value, SIDE, 1)

    def take(source, own, after, grant):
        return take_stage(place, source, own, after, grant)

    give_in = take(expert_in, False, place, GIVE_GRANTS[0])
    other_in = share(give_in)
    block = jax.ShapeDtypeStruct((rows + META, half), BF16)
    mine, theirs = kernel(
        norm_kernel, give_in, [block] * 2,
        place, tokens, expert_ids.T, gate_weights.T,
    )
    peer = cross(theirs)
    own_in = take(expert_in, True, mine, GIVE_GRANTS[1])
    far = far_groups(groups)
    feeds = {"o": [mine, peer]}
    feeds["n"] = [swap(mine, GROUP, 1), swap(peer, GROUP, 1)]
    for g in far:
        if g % 2:
            early = swap(mine, GROUP, g)
            got = pair_up(early, swap(peer, GROUP, g), rows)
        else:
            got = swap(feeds[str(g + 1)][0], GROUP, 1)
        feeds[str(g)] = [got, share(got)]
    if far:
        feeds["m"] = [feeds["2"].pop()]

    firsts, kept, sums = {}, {}, []
    last, own_out = own_in, None

    def first(g):
        nonlocal last
        part, code, gate, *pair = first_stage(feeds[g], rows, place, own_in, other_in, last, picks)
        firsts[g] = (part, code, gate, cross(part))
        last = code
        return pair

    def second(g):
        nonlocal last, own_out
        part, code, gate, across = firsts[g]
        load = own_out is None
        keep, send, join = g not in "ltm2", g not in "on2", g == "2"
        outs = second_stage(
            code.shape[1] // (2 * rows), code, gate, part, across, place, expert_out if load else own_out,
            other_out, kept["m"] if join else last, keep, send, join, load,
        )
        last = outs[0]
        own_out = outs[-1] if load else own_out
        if keep:
            kept[g] = outs[0]
        if join:
            sums.append(swap(last, GROUP, 2).astype(F32))
        if not send:
            return
        came = share(outs[keep])
        if g == "m":
            kept[g] = came
            return
        came = came.astype(F32)
        if g != "t":
            last = (kept.pop("n" if g == "l" else g) + came).astype(BF16)
            came = swap(last, GROUP, 1 if g == "l" else int(g)).astype(F32)
        sums.append(came)

    (unit,) = first("o")
    feeds["t"] = [share(unit)]
    last = give_out = take(expert_out, False, last, GIVE_GRANTS[2])
    other_out = share(give_out)
    other_shared_in = share(shared_in)
    other_shared_out = share(shared_out)
    tail = [str(g) for g in far[:-1]] + ["m", "2"] * bool(far)
    (near,) = first("n")
    feeds["l"] = [share(near)]
    first("l")
    second("o")
    for g in tail[:1]:
        first(g)
    second("n")
    second("l")
    for g in tail[1:]:
        first(g)
    first("t")
    (shared_part,) = kernel(
        shared_first_kernel, last,
        [jax.ShapeDtypeStruct((2 * rows, hidden), BF16)],
        place, unit, shared_in, other_shared_in,
    )
    last = shared_part
    shared_far = cross(shared_part)
    for g in [*tail, "t"]:
        second(g)
    (shared,) = kernel(
        shared_second_kernel, last,
        [jax.ShapeDtypeStruct((2 * rows, half), F32)],
        place, shared_part, shared_far, shared_out, other_shared_out,
    )

    total = sum(sums, shared + kept["o"])
    crossed = cross(total[rows:].astype(BF16)).astype(F32)
    stay = total[:rows]
    low = side == 0
    added = jnp.concatenate([jnp.where(low, stay, crossed), jnp.where(low, crossed, stay)], axis=1)
    return (tokens.astype(F32) + added).astype(BF16)


def exchange_fits(mesh, tokens, expert_ids, expert_in):
    groups, sides = mesh.shape[GROUP], mesh.shape[SIDE]
    blocks = mesh.shape[SWEEP] * groups
    rows, width = tokens.shape[0] // (blocks * sides), tokens.shape[1]
    return (
        sides == 4
        and expert_in.shape[0] % (blocks * 16) == 0
        and groups in (4, 8)
        and rows % 128 == 0
        and width % 512 == 0
        and width // 2 >= 3 * rows
        and expert_ids.shape[1] <= META
        and expert_in.shape[2] % 128 == 0
    )


def pair_up(first, second, rows):
    return jnp.concatenate([first[:rows], second[:rows], first[rows:], second[rows:]], axis=0)


def far_groups(groups):
    return list(range(groups - 1, 1, -1))


def solution(mesh):
    rows = P((SWEEP, GROUP, SIDE), None)
    placed = (
        rows,
        rows,
        rows,
        P((SWEEP, GROUP), SIDE, None),
        P((SWEEP, GROUP), None, SIDE),
        P((SWEEP, SIDE), None),
        P(SWEEP, SIDE),
    )
    spread = functools.partial(
        jax.shard_map, mesh=mesh, in_specs=placed, out_specs=rows, check_vma=False
    )

    def program(*args):
        if not exchange_fits(mesh, args[0], args[1], args[3]):
            return spread(gathered_weights)(*args)
        step = spread(exchanged_partials)
        return step(*args)

    return program
```

```python
import functools

import jax
import jax.numpy as jnp
from jax import lax
from jax.experimental import pallas as pl
from jax.experimental.pallas import tpu as pltpu
from jax.sharding import PartitionSpec as P


CAP = 20
STEP = 4
SWEEP, GROUP, SIDE = "sweep", "expert", "dp"
F32 = jnp.float32
BF16 = jnp.bfloat16
KERNEL_FLOPS = 10_000_000
META = 8


def layer_norm(tokens):
    values = tokens.astype(F32)
    center = values - jnp.mean(values, axis=-1, keepdims=True)
    spread = jnp.mean(center * center, axis=-1, keepdims=True)
    return (center * lax.rsqrt(spread + 1e-06)).astype(BF16)


def copy_slots(expert_ids, expert_count):
    expert_iota = jnp.arange(expert_count, dtype=jnp.int32)
    matches = (expert_ids[..., None] == expert_iota).astype(jnp.int32)
    per_token = jnp.sum(matches, axis=-2, dtype=jnp.int32)
    earlier = jnp.cumsum(per_token, axis=-2, dtype=jnp.int32) - per_token
    return jnp.sum(matches * earlier[..., None, :], axis=-1, dtype=jnp.int32)


def run_experts(shard_piece, weight_in, weight_out):
    pre_act = jnp.einsum("gesd,edf->gesf", shard_piece, weight_in, preferred_element_type=F32)
    hidden = jax.nn.gelu(pre_act).astype(BF16)
    return jnp.einsum("gesf,efd->gesd", hidden, weight_out, preferred_element_type=F32).astype(BF16)


def gathered_weights(tokens, expert_ids, gate_weights, expert_in, expert_out, shared_in, shared_out):
    row_count, model_width = tokens.shape
    pick_count = expert_ids.shape[1]
    local_count = expert_in.shape[0]
    group_count = lax.axis_size(GROUP)
    expert_total = local_count * group_count
    normed = layer_norm(tokens)
    full_in = lax.all_gather(expert_in, SIDE, axis=1, tiled=True)
    full_out = lax.all_gather(expert_out, SIDE, axis=2, tiled=True)
    slot_of = copy_slots(expert_ids, expert_total)
    positions = (expert_ids * CAP + slot_of).reshape(-1)
    copies = jnp.repeat(normed, pick_count, axis=0)
    outgoing = jnp.zeros((expert_total * CAP, model_width), BF16).at[positions].set(copies)
    outgoing = outgoing.reshape(group_count, local_count, CAP, model_width)
    received = lax.all_to_all(outgoing, GROUP, split_axis=0, concat_axis=0, tiled=True)
    returned = lax.all_to_all(
        run_experts(received, full_in, full_out), GROUP, split_axis=0, concat_axis=0, tiled=True
    )
    results = returned.reshape(expert_total * CAP, model_width)[positions].reshape(
        row_count, pick_count, model_width
    )
    routed = jnp.sum(results.astype(F32) * gate_weights[:, :, None], axis=1)
    shared_pre = jnp.dot(
        normed, lax.all_gather(shared_in, SIDE, axis=0, tiled=True), preferred_element_type=F32
    )
    shared_hidden = jax.nn.gelu(shared_pre).astype(BF16)
    shared_result = jnp.dot(
        shared_hidden,
        lax.all_gather(shared_out, SIDE, axis=1, tiled=True),
        preferred_element_type=F32,
    )
    return (tokens.astype(F32) + shared_result + routed).astype(BF16)


def dot(a, b):
    return jnp.dot(a, b, preferred_element_type=F32)


def cost(flops, moved):
    return pl.CostEstimate(flops=int(flops), bytes_accessed=int(moved), transcendentals=0)


def half_copies(source, held, base, came):
    return [
        pltpu.make_async_copy(source.at[base + e], held.at[e], came.at[e])
        for e in range(held.shape[0])
    ]


def norm_kernel(place, tokens, ids, gates, _, mine, theirs):
    rows, width = tokens.shape
    half = width // 2
    values = tokens[...].astype(F32)
    center = values - jnp.mean(values, axis=-1, keepdims=True)
    spread = jnp.mean(center * center, axis=-1, keepdims=True)
    normed = (center * lax.rsqrt(spread + 1e-06)).astype(BF16)
    low = place[1] == 0
    mine[0:rows, :] = jnp.where(low, normed[:, :half], normed[:, half:])
    theirs[0:rows, :] = jnp.where(low, normed[:, half:], normed[:, :half])
    gate = gates[...]
    high = gate.astype(BF16).astype(F32)
    rest = gate - high
    picks = ids.shape[0]
    spare = jnp.zeros((picks, half - 3 * rows), F32)
    table = jnp.concatenate([ids[...].astype(F32), high, rest, spare], axis=1)
    if picks < META:
        table = jnp.concatenate([table, jnp.zeros((META - picks, half), F32)], axis=0)
    table = table.astype(BF16)
    mine[rows : rows + META, :] = table
    theirs[rows : rows + META, :] = table


def take_kernel(own, place, source, after, taken, came):
    local = taken.shape[0]
    copies = half_copies(source, taken, (place[0] if own else 1 - place[0]) * local, came)
    for c in copies:
        c.start()
    for c in copies:
        c.wait()


def selection(codes, rows):
    count, tokens = codes.shape
    wanted = lax.broadcasted_iota(jnp.int32, (rows, tokens), 0).astype(F32)
    return [(wanted == codes[e : e + 1, :]).astype(F32) for e in range(count)]


def first_kernel(feed_count, tokens, picks, place, *refs):
    feeds, refs = refs[:feed_count], refs[feed_count:]
    own, other, _, part, code, gate, *pair, packed = refs
    local, rows, half = packed.shape
    block_counts = [feed.shape[0] // (tokens + META) for feed in feeds]
    for unit in pair:
        for b, feed in enumerate(feeds):
            at = len(feeds) * tokens + b * META
            unit[b * tokens : (b + 1) * tokens, :] = feed[0:tokens, :]
            unit[at : at + META, :] = feed[tokens:, :]
    slots = rows // sum(block_counts)
    before = (
        lax.broadcasted_iota(jnp.int32, (tokens, tokens), 0)
        < lax.broadcasted_iota(jnp.int32, (tokens, tokens), 1)
    ).astype(F32).astype(BF16)
    expert = (lax.broadcasted_iota(jnp.int32, (local, tokens), 0) + place[2]).astype(F32)
    tables = [
        feed[count * tokens + b * META : count * tokens + (b + 1) * META, 0 : 3 * tokens]
        for feed, count in zip(feeds, block_counts)
        for b in range(count)
    ]
    for i, table in enumerate(tables):
        table = table.astype(F32)
        named = jnp.zeros((local, tokens), F32)
        weight = jnp.zeros((local, tokens), F32)
        for k in range(picks):
            same = table[k : k + 1, 0:tokens] == expert
            value = table[k : k + 1, tokens : 2 * tokens] + table[k : k + 1, 2 * tokens :]
            named = jnp.where(same, 1.0, named)
            weight = jnp.where(same, value, weight)
        rank = dot(named.astype(BF16), before)
        turn = 1 - place[1] if i % 2 else place[1]
        base = ((i - i % 2 + turn) * slots).astype(F32)
        column = i * tokens
        code[:, column : column + tokens] = jnp.where(named > 0, rank + base, -1.0)
        gate[:, column : column + tokens] = weight
    pick = jnp.concatenate(selection(code[...], rows), axis=0).astype(BF16)
    wide = half // 3 if half % 384 == 0 else half
    for n in range(half // wide):
        columns = slice(n * wide, (n + 1) * wide)
        chosen, column = 0.0, 0
        for feed, count in zip(feeds, block_counts):
            held = slice(column, column + count * tokens)
            chosen += dot(pick[:, held], feed[0 : count * tokens, columns])
            column += count * tokens
        for e in range(local):
            packed[e, :, columns] = chosen[e * rows : (e + 1) * rows].astype(BF16)

    quarter = half // 2
    here = pl.multiple_of(place[0] * quarter, quarter)
    there = pl.multiple_of((1 - place[0]) * quarter, quarter)

    @pl.loop(0, local // STEP)
    def _(turn):
        for e in [STEP * turn + i for i in range(STEP)]:
            total = dot(packed[e, :, pl.ds(here, quarter)], own[e])
            total += dot(packed[e, :, pl.ds(there, quarter)], other[e])
            part[e] = total.astype(BF16)


def second_kernel(units, keep, send, join, load, place, *refs):
    code, gate, near, far, source, other, after = refs[:7]
    shown = keep + send + join
    outs, refs = refs[7 : 7 + shown], refs[7 + shown :]
    own, (total, *came) = (refs[0], refs[1:]) if load else (source, refs)
    local = code.shape[0]
    rows = near.shape[1]
    half = total.shape[1]
    if load:
        for c in half_copies(source, own, place[0] * local, came[0]):
            c.start()
    quarter = half // 2
    here = pl.multiple_of(place[0] * quarter, quarter)
    there = pl.multiple_of((1 - place[0]) * quarter, quarter)
    wanted = lax.broadcasted_iota(jnp.int32, (rows, code.shape[1]), 0).astype(F32)

    @pl.loop(0, local // STEP)
    def _(turn):
        for e in [STEP * turn + i for i in range(STEP)]:
            same = wanted == code[pl.ds(e, 1), :]
            scale = jnp.sum(jnp.where(same, gate[pl.ds(e, 1), :], 0.0), axis=1, keepdims=True)
            hidden = jax.nn.gelu(near[e].astype(F32) + far[e].astype(F32)).astype(BF16)
            at = pl.ds(pl.multiple_of(e * rows, rows), rows)
            total[at, pl.ds(there, quarter)] = dot(hidden, other[e]) * scale
            if load:
                base = place[0] * local
                pltpu.make_async_copy(source.at[base + e], own.at[e], came[0].at[e]).wait()
            total[at, pl.ds(here, quarter)] = dot(hidden, own[e]) * scale

    pick = jnp.concatenate(selection(code[...], rows), axis=0).astype(BF16)
    wide = half // 3 if half % 384 == 0 else half
    count = code.shape[1] // units
    for n in range(half // wide):
        columns = slice(n * wide, (n + 1) * wide)
        summed = lax.dot_general(
            pick,
            total[:, columns].astype(BF16),
            (((0,), (0,)), ((), ())),
            preferred_element_type=F32,
        )
        slot = 0
        if keep:
            outs[slot][:, columns] = summed[0:count]
            slot += 1
        if send:
            outs[slot][:, columns] = summed[(units - 1) * count :].astype(BF16)
        if join:
            outs[slot][:, columns] = (summed + after[:, columns].astype(F32)).astype(BF16)


SMEM = pl.BlockSpec(memory_space=pltpu.SMEM)
VMEM = pl.BlockSpec(memory_space=pltpu.VMEM)
ANY = pl.BlockSpec(memory_space=pl.ANY)
HBM = pl.BlockSpec(memory_space=pltpu.HBM)
GRANT = 24 << 20
GIVE_GRANTS = (46 << 20, 41 << 20, 41 << 20)
SECOND_GRANT = 35 << 20


def granted(size=GRANT):
    return pltpu.CompilerParams(vmem_limit_bytes=size)


def first_stage(feeds, tokens, place, own, other, after, picks):
    local, quarter, hidden = other.shape
    half = 2 * quarter
    blocks = sum(feed.shape[0] for feed in feeds) // (tokens + META)
    rows = blocks * CAP
    pair = [jax.ShapeDtypeStruct((blocks * (tokens + META), half), BF16)] * (len(feeds) == blocks)
    table = jax.ShapeDtypeStruct((local, blocks * tokens), F32)
    return pl.pallas_call(
        functools.partial(first_kernel, len(feeds), tokens, picks),
        in_specs=[SMEM] + [VMEM] * (len(feeds) + 2) + [ANY],
        out_specs=[VMEM] * (3 + len(pair)),
        scratch_shapes=[pltpu.VMEM((local, rows, half), BF16)],
        out_shape=[jax.ShapeDtypeStruct((local, rows, hidden), BF16), table, table, *pair],
        compiler_params=granted(),
        cost_estimate=cost(KERNEL_FLOPS, 2 * local * half * hidden),
    )(place, *feeds, own, other, after)


def second_stage(units, code, gate, near, far, place, own, other, after, keep, send, join, load):
    local, hidden, quarter = other.shape
    half = 2 * quarter
    rows = near.shape[1]
    count = code.shape[1] // units
    shapes = []
    if keep:
        shapes.append(jax.ShapeDtypeStruct((count, half), F32))
    if send or join:
        shapes.append(jax.ShapeDtypeStruct((count, half), BF16))
    if load:
        shapes.append(jax.ShapeDtypeStruct(other.shape, BF16))
    return pl.pallas_call(
        functools.partial(second_kernel, units, keep, send, join, load),
        in_specs=[SMEM] + [VMEM] * 4 + [HBM if load else VMEM, VMEM, VMEM if join else ANY],
        out_specs=[VMEM] * len(shapes),
        scratch_shapes=[pltpu.VMEM((local * rows, half), F32)]
        + [pltpu.SemaphoreType.DMA((local,))] * load,
        out_shape=shapes,
        compiler_params=granted(SECOND_GRANT if load else GRANT),
        cost_estimate=cost(KERNEL_FLOPS, 2 * local * half * hidden),
    )(place, code, gate, near, far, own, other, after)


def shared_first_kernel(place, feed, own, other, _, part):
    quarter = own.shape[0]
    rows = part.shape[0] // 2
    here = pl.multiple_of(place[0] * quarter, quarter)
    there = pl.multiple_of((1 - place[0]) * quarter, quarter)
    total = dot(feed[0 : 2 * rows, pl.ds(here, quarter)], own[...])
    total += dot(feed[0 : 2 * rows, pl.ds(there, quarter)], other[...])
    for b in range(2):
        turn = place[1] if b == 0 else 1 - place[1]
        at = pl.ds(pl.multiple_of(turn * rows, rows), rows)
        part[at, :] = total[b * rows : (b + 1) * rows].astype(BF16)


def shared_second_kernel(place, near, far, own, other, _, out):
    quarter = own.shape[1]
    rows = near.shape[0] // 2
    here = pl.multiple_of(place[0] * quarter, quarter)
    there = pl.multiple_of((1 - place[0]) * quarter, quarter)
    hidden = jax.nn.gelu(near[...].astype(F32) + far[...].astype(F32)).astype(BF16)
    left, right = dot(hidden, own[...]), dot(hidden, other[...])
    for b in range(2):
        turn = place[1] if b == 0 else 1 - place[1]
        at = pl.ds(pl.multiple_of(turn * rows, rows), rows)
        out[at, pl.ds(here, quarter)] = left[b * rows : (b + 1) * rows]
        out[at, pl.ds(there, quarter)] = right[b * rows : (b + 1) * rows]


def take_stage(place, source, own, after, grant):
    shape = (source.shape[0] // 2, *source.shape[1:])
    return pl.pallas_call(
        functools.partial(take_kernel, own),
        in_specs=[SMEM, HBM, ANY],
        out_specs=VMEM,
        out_shape=jax.ShapeDtypeStruct(shape, BF16),
        scratch_shapes=[pltpu.SemaphoreType.DMA(shape[:1])],
        compiler_params=granted(grant),
        cost_estimate=cost(KERNEL_FLOPS, 4 * shape[0] * shape[1] * shape[2]),
    )(place, source, after)


def kernel(body, after, shapes, place, *args):
    return pl.pallas_call(
        body,
        in_specs=[SMEM] + [VMEM] * len(args) + [ANY],
        out_specs=[VMEM] * len(shapes),
        out_shape=shapes,
        compiler_params=granted(),
        cost_estimate=cost(KERNEL_FLOPS, 1 << 20),
    )(place, *args, after)


def exchanged_partials(tokens, expert_ids, gate_weights, expert_in, expert_out, shared_in, shared_out):
    rows, width = tokens.shape
    half = width // 2
    picks = expert_ids.shape[1]
    group = expert_in.shape[0]
    local = group // 2
    hidden = expert_in.shape[2]
    groups = lax.axis_size(GROUP)
    spot = lax.axis_index(SIDE)
    side, core = spot // 2, spot % 2
    lead = lax.axis_index(GROUP) * group + core * local
    place = jnp.stack([core, side, lead]).astype(jnp.int32)

    def swap(value, axis, mask):
        return lax.ppermute(value, axis, [(i, i ^ mask) for i in range(lax.axis_size(axis))])

    def cross(value):
        return swap(value, SIDE, 2)

    def share(value):
        return swap(value, SIDE, 1)

    def take(source, own, after, grant):
        return take_stage(place, source, own, after, grant)

    give_in = take(expert_in, False, place, GIVE_GRANTS[0])
    other_in = share(give_in)
    block = jax.ShapeDtypeStruct((rows + META, half), BF16)
    mine, theirs = kernel(
        norm_kernel, give_in, [block] * 2,
        place, tokens, expert_ids.T, gate_weights.T,
    )
    peer = cross(theirs)
    own_in = take(expert_in, True, mine, GIVE_GRANTS[1])
    far = far_groups(groups)
    feeds = {"o": [mine, peer]}
    feeds["n"] = [swap(mine, GROUP, 1), swap(peer, GROUP, 1)]
    for g in far:
        if g % 2:
            early = swap(mine, GROUP, g)
            got = pair_up(early, swap(peer, GROUP, g), rows)
        else:
            got = swap(feeds[str(g + 1)][0], GROUP, 1)
        feeds[str(g)] = [got, share(got)]
    if far:
        feeds["m"] = [feeds["2"].pop()]

    firsts, kept, sums = {}, {}, []
    last, own_out = own_in, None

    def first(g):
        nonlocal last
        part, code, gate, *pair = first_stage(feeds[g], rows, place, own_in, other_in, last, picks)
        firsts[g] = (part, code, gate, cross(part))
        last = code
        return pair

    def second(g):
        nonlocal last, own_out
        part, code, gate, across = firsts[g]
        load = own_out is None
        keep, send, join = g not in "ltm2", g not in "on2", g == "2"
        outs = second_stage(
            code.shape[1] // (2 * rows), code, gate, part, across, place, expert_out if load else own_out,
            other_out, kept["m"] if join else last, keep, send, join, load,
        )
        last = outs[0]
        own_out = outs[-1] if load else own_out
        if keep:
            kept[g] = outs[0]
        if join:
            sums.append(swap(last, GROUP, 2).astype(F32))
        if not send:
            return
        came = share(outs[keep])
        if g == "m":
            kept[g] = came
            return
        came = came.astype(F32)
        if g != "t":
            last = (kept.pop("n" if g == "l" else g) + came).astype(BF16)
            came = swap(last, GROUP, 1 if g == "l" else int(g)).astype(F32)
        sums.append(came)

    (unit,) = first("o")
    feeds["t"] = [share(unit)]
    last = give_out = take(expert_out, False, last, GIVE_GRANTS[2])
    other_out = share(give_out)
    other_shared_in = share(shared_in)
    other_shared_out = share(shared_out)
    tail = [str(g) for g in far[:-1]] + ["m", "2"] * bool(far)
    (near,) = first("n")
    feeds["l"] = [share(near)]
    first("l")
    second("o")
    for g in tail[:1]:
        first(g)
    second("n")
    second("l")
    for g in tail[1:]:
        first(g)
    first("t")
    (shared_part,) = kernel(
        shared_first_kernel, last,
        [jax.ShapeDtypeStruct((2 * rows, hidden), BF16)],
        place, unit, shared_in, other_shared_in,
    )
    last = shared_part
    shared_far = cross(shared_part)
    for g in [*tail, "t"]:
        second(g)
    (shared,) = kernel(
        shared_second_kernel, last,
        [jax.ShapeDtypeStruct((2 * rows, half), F32)],
        place, shared_part, shared_far, shared_out, other_shared_out,
    )

    total = sum(sums, shared + kept["o"])
    crossed = cross(total[rows:].astype(BF16)).astype(F32)
    stay = total[:rows]
    low = side == 0
    added = jnp.concatenate([jnp.where(low, stay, crossed), jnp.where(low, crossed, stay)], axis=1)
    return (tokens.astype(F32) + added).astype(BF16)


def exchange_fits(mesh, tokens, expert_ids, expert_in):
    groups, sides = mesh.shape[GROUP], mesh.shape[SIDE]
    blocks = mesh.shape[SWEEP] * groups
    rows, width = tokens.shape[0] // (blocks * sides), tokens.shape[1]
    return (
        sides == 4
        and expert_in.shape[0] % (blocks * 16) == 0
        and groups in (4, 8)
        and rows % 128 == 0
        and width % 512 == 0
        and width // 2 >= 3 * rows
        and expert_ids.shape[1] <= META
        and expert_in.shape[2] % 128 == 0
    )


def pair_up(first, second, rows):
    return jnp.concatenate([first[:rows], second[:rows], first[rows:], second[rows:]], axis=0)


def far_groups(groups):
    return list(range(groups - 1, 1, -1))


def solution(mesh):
    rows = P((SWEEP, GROUP, SIDE), None)
    placed = (
        rows,
        rows,
        rows,
        P((SWEEP, GROUP), SIDE, None),
        P((SWEEP, GROUP), None, SIDE),
        P((SWEEP, SIDE), None),
        P(SWEEP, SIDE),
    )
    spread = functools.partial(
        jax.shard_map, mesh=mesh, in_specs=placed, out_specs=rows, check_vma=False
    )

    def program(*args):
        if not exchange_fits(mesh, args[0], args[1], args[3]):
            return spread(gathered_weights)(*args)
        step = spread(exchanged_partials)
        return step(*args)

    return program
```

```python
import functools

import jax
import jax.numpy as jnp
from jax import lax
from jax.experimental import pallas as pl
from jax.experimental.pallas import tpu as pltpu
from jax.sharding import PartitionSpec as P


CAP = 20
STEP = 4
SWEEP, GROUP, SIDE = "sweep", "expert", "dp"
F32 = jnp.float32
BF16 = jnp.bfloat16
KERNEL_FLOPS = 10_000_000
META = 8


def layer_norm(tokens):
    values = tokens.astype(F32)
    center = values - jnp.mean(values, axis=-1, keepdims=True)
    spread = jnp.mean(center * center, axis=-1, keepdims=True)
    return (center * lax.rsqrt(spread + 1e-06)).astype(BF16)


def copy_slots(expert_ids, expert_count):
    expert_iota = jnp.arange(expert_count, dtype=jnp.int32)
    matches = (expert_ids[..., None] == expert_iota).astype(jnp.int32)
    per_token = jnp.sum(matches, axis=-2, dtype=jnp.int32)
    earlier = jnp.cumsum(per_token, axis=-2, dtype=jnp.int32) - per_token
    return jnp.sum(matches * earlier[..., None, :], axis=-1, dtype=jnp.int32)


def run_experts(shard_piece, weight_in, weight_out):
    pre_act = jnp.einsum("gesd,edf->gesf", shard_piece, weight_in, preferred_element_type=F32)
    hidden = jax.nn.gelu(pre_act).astype(BF16)
    return jnp.einsum("gesf,efd->gesd", hidden, weight_out, preferred_element_type=F32).astype(BF16)


def gathered_weights(tokens, expert_ids, gate_weights, expert_in, expert_out, shared_in, shared_out):
    row_count, model_width = tokens.shape
    pick_count = expert_ids.shape[1]
    local_count = expert_in.shape[0]
    group_count = lax.axis_size(GROUP)
    expert_total = local_count * group_count
    normed = layer_norm(tokens)
    full_in = lax.all_gather(expert_in, SIDE, axis=1, tiled=True)
    full_out = lax.all_gather(expert_out, SIDE, axis=2, tiled=True)
    slot_of = copy_slots(expert_ids, expert_total)
    positions = (expert_ids * CAP + slot_of).reshape(-1)
    copies = jnp.repeat(normed, pick_count, axis=0)
    outgoing = jnp.zeros((expert_total * CAP, model_width), BF16).at[positions].set(copies)
    outgoing = outgoing.reshape(group_count, local_count, CAP, model_width)
    received = lax.all_to_all(outgoing, GROUP, split_axis=0, concat_axis=0, tiled=True)
    returned = lax.all_to_all(
        run_experts(received, full_in, full_out), GROUP, split_axis=0, concat_axis=0, tiled=True
    )
    results = returned.reshape(expert_total * CAP, model_width)[positions].reshape(
        row_count, pick_count, model_width
    )
    routed = jnp.sum(results.astype(F32) * gate_weights[:, :, None], axis=1)
    shared_pre = jnp.dot(
        normed, lax.all_gather(shared_in, SIDE, axis=0, tiled=True), preferred_element_type=F32
    )
    shared_hidden = jax.nn.gelu(shared_pre).astype(BF16)
    shared_result = jnp.dot(
        shared_hidden,
        lax.all_gather(shared_out, SIDE, axis=1, tiled=True),
        preferred_element_type=F32,
    )
    return (tokens.astype(F32) + shared_result + routed).astype(BF16)


def dot(a, b):
    return jnp.dot(a, b, preferred_element_type=F32)


def cost(flops, moved):
    return pl.CostEstimate(flops=int(flops), bytes_accessed=int(moved), transcendentals=0)


def half_copies(source, held, base, came):
    return [
        pltpu.make_async_copy(source.at[base + e], held.at[e], came.at[e])
        for e in range(held.shape[0])
    ]


def norm_kernel(place, tokens, ids, gates, _, mine, theirs):
    rows, width = tokens.shape
    half = width // 2
    values = tokens[...].astype(F32)
    center = values - jnp.mean(values, axis=-1, keepdims=True)
    spread = jnp.mean(center * center, axis=-1, keepdims=True)
    normed = (center * lax.rsqrt(spread + 1e-06)).astype(BF16)
    low = place[1] == 0
    mine[0:rows, :] = jnp.where(low, normed[:, :half], normed[:, half:])
    theirs[0:rows, :] = jnp.where(low, normed[:, half:], normed[:, :half])
    gate = gates[...]
    high = gate.astype(BF16).astype(F32)
    rest = gate - high
    picks = ids.shape[0]
    spare = jnp.zeros((picks, half - 3 * rows), F32)
    table = jnp.concatenate([ids[...].astype(F32), high, rest, spare], axis=1)
    if picks < META:
        table = jnp.concatenate([table, jnp.zeros((META - picks, half), F32)], axis=0)
    table = table.astype(BF16)
    mine[rows : rows + META, :] = table
    theirs[rows : rows + META, :] = table


def take_kernel(own, lead, place, source, after, taken, came):
    local = source.shape[0] // 2
    copies = half_copies(source, taken, (place[0] if own else 1 - place[0]) * local + lead, came)
    for c in copies:
        c.start()
    for c in copies:
        c.wait()


def selection(codes, rows):
    count, tokens = codes.shape
    wanted = lax.broadcasted_iota(jnp.int32, (rows, tokens), 0).astype(F32)
    return [(wanted == codes[e : e + 1, :]).astype(F32) for e in range(count)]


def first_kernel(feed_count, tokens, picks, place, *refs):
    feeds, refs = refs[:feed_count], refs[feed_count:]
    own, low, high, _, part, code, gate, *pair, packed = refs
    local, rows, half = packed.shape
    block_counts = [feed.shape[0] // (tokens + META) for feed in feeds]
    for unit in pair:
        for b, feed in enumerate(feeds):
            at = len(feeds) * tokens + b * META
            unit[b * tokens : (b + 1) * tokens, :] = feed[0:tokens, :]
            unit[at : at + META, :] = feed[tokens:, :]
    slots = rows // sum(block_counts)
    before = (
        lax.broadcasted_iota(jnp.int32, (tokens, tokens), 0)
        < lax.broadcasted_iota(jnp.int32, (tokens, tokens), 1)
    ).astype(F32).astype(BF16)
    expert = (lax.broadcasted_iota(jnp.int32, (local, tokens), 0) + place[2]).astype(F32)
    tables = [
        feed[count * tokens + b * META : count * tokens + (b + 1) * META, 0 : 3 * tokens]
        for feed, count in zip(feeds, block_counts)
        for b in range(count)
    ]
    for i, table in enumerate(tables):
        table = table.astype(F32)
        named = jnp.zeros((local, tokens), F32)
        weight = jnp.zeros((local, tokens), F32)
        for k in range(picks):
            same = table[k : k + 1, 0:tokens] == expert
            value = table[k : k + 1, tokens : 2 * tokens] + table[k : k + 1, 2 * tokens :]
            named = jnp.where(same, 1.0, named)
            weight = jnp.where(same, value, weight)
        rank = dot(named.astype(BF16), before)
        turn = 1 - place[1] if i % 2 else place[1]
        base = ((i - i % 2 + turn) * slots).astype(F32)
        column = i * tokens
        code[:, column : column + tokens] = jnp.where(named > 0, rank + base, -1.0)
        gate[:, column : column + tokens] = weight
    pick = jnp.concatenate(selection(code[...], rows), axis=0).astype(BF16)
    wide = half // 3 if half % 384 == 0 else half
    for n in range(half // wide):
        columns = slice(n * wide, (n + 1) * wide)
        chosen, column = 0.0, 0
        for feed, count in zip(feeds, block_counts):
            held = slice(column, column + count * tokens)
            chosen += dot(pick[:, held], feed[0 : count * tokens, columns])
            column += count * tokens
        for e in range(local):
            packed[e, :, columns] = chosen[e * rows : (e + 1) * rows].astype(BF16)

    quarter = half // 2
    here = pl.multiple_of(place[0] * quarter, quarter)
    there = pl.multiple_of((1 - place[0]) * quarter, quarter)

    for e in range(local):
        other = low if e < local // 2 else high
        total = dot(packed[e, :, pl.ds(here, quarter)], own[e])
        total += dot(packed[e, :, pl.ds(there, quarter)], other[e % (local // 2)])
        part[e] = total.astype(BF16)


def second_kernel(units, keep, send, join, load, place, *refs):
    code, gate, near, far, source, other, after = refs[:7]
    shown = keep + send + join
    outs, refs = refs[7 : 7 + shown], refs[7 + shown :]
    own, (total, *came) = (refs[0], refs[1:]) if load else (source, refs)
    local = code.shape[0]
    rows = near.shape[1]
    half = total.shape[1]
    if load:
        for c in half_copies(source, own, place[0] * local, came[0]):
            c.start()
    quarter = half // 2
    here = pl.multiple_of(place[0] * quarter, quarter)
    there = pl.multiple_of((1 - place[0]) * quarter, quarter)
    wanted = lax.broadcasted_iota(jnp.int32, (rows, code.shape[1]), 0).astype(F32)

    @pl.loop(0, local // STEP)
    def _(turn):
        for e in [STEP * turn + i for i in range(STEP)]:
            same = wanted == code[pl.ds(e, 1), :]
            scale = jnp.sum(jnp.where(same, gate[pl.ds(e, 1), :], 0.0), axis=1, keepdims=True)
            hidden = jax.nn.gelu(near[e].astype(F32) + far[e].astype(F32)).astype(BF16)
            at = pl.ds(pl.multiple_of(e * rows, rows), rows)
            total[at, pl.ds(there, quarter)] = dot(hidden, other[e]) * scale
            if load:
                base = place[0] * local
                pltpu.make_async_copy(source.at[base + e], own.at[e], came[0].at[e]).wait()
            total[at, pl.ds(here, quarter)] = dot(hidden, own[e]) * scale

    pick = jnp.concatenate(selection(code[...], rows), axis=0).astype(BF16)
    wide = half // 3 if half % 384 == 0 else half
    count = code.shape[1] // units
    for n in range(half // wide):
        columns = slice(n * wide, (n + 1) * wide)
        summed = lax.dot_general(
            pick,
            total[:, columns].astype(BF16),
            (((0,), (0,)), ((), ())),
            preferred_element_type=F32,
        )
        slot = 0
        if keep:
            outs[slot][:, columns] = summed[0:count]
            slot += 1
        if send:
            outs[slot][:, columns] = summed[(units - 1) * count :].astype(BF16)
        if join:
            outs[slot][:, columns] = (summed + after[:, columns].astype(F32)).astype(BF16)


SMEM = pl.BlockSpec(memory_space=pltpu.SMEM)
VMEM = pl.BlockSpec(memory_space=pltpu.VMEM)
ANY = pl.BlockSpec(memory_space=pl.ANY)
HBM = pl.BlockSpec(memory_space=pltpu.HBM)
GRANT = 24 << 20
GIVE_GRANTS = (46 << 20, 42 << 20, 41 << 20)
SECOND_GRANT = 35 << 20


def granted(size=GRANT):
    return pltpu.CompilerParams(vmem_limit_bytes=size)


def first_stage(feeds, tokens, place, own, other, after, picks):
    local, quarter, hidden = own.shape
    half = 2 * quarter
    blocks = sum(feed.shape[0] for feed in feeds) // (tokens + META)
    rows = blocks * CAP
    pair = [jax.ShapeDtypeStruct((blocks * (tokens + META), half), BF16)] * (len(feeds) == blocks)
    table = jax.ShapeDtypeStruct((local, blocks * tokens), F32)
    return pl.pallas_call(
        functools.partial(first_kernel, len(feeds), tokens, picks),
        in_specs=[SMEM] + [VMEM] * (len(feeds) + 3) + [ANY],
        out_specs=[VMEM] * (3 + len(pair)),
        scratch_shapes=[pltpu.VMEM((local, rows, half), BF16)],
        out_shape=[jax.ShapeDtypeStruct((local, rows, hidden), BF16), table, table, *pair],
        compiler_params=granted(),
        cost_estimate=cost(KERNEL_FLOPS, 2 * local * half * hidden),
    )(place, *feeds, own, *other, after)


def second_stage(units, code, gate, near, far, place, own, other, after, keep, send, join, load):
    local, hidden, quarter = other.shape
    half = 2 * quarter
    rows = near.shape[1]
    count = code.shape[1] // units
    shapes = []
    if keep:
        shapes.append(jax.ShapeDtypeStruct((count, half), F32))
    if send or join:
        shapes.append(jax.ShapeDtypeStruct((count, half), BF16))
    if load:
        shapes.append(jax.ShapeDtypeStruct(other.shape, BF16))
    return pl.pallas_call(
        functools.partial(second_kernel, units, keep, send, join, load),
        in_specs=[SMEM] + [VMEM] * 4 + [HBM if load else VMEM, VMEM, VMEM if join else ANY],
        out_specs=[VMEM] * len(shapes),
        scratch_shapes=[pltpu.VMEM((local * rows, half), F32)]
        + [pltpu.SemaphoreType.DMA((local,))] * load,
        out_shape=shapes,
        compiler_params=granted(SECOND_GRANT if load else GRANT),
        cost_estimate=cost(KERNEL_FLOPS, 2 * local * half * hidden),
    )(place, code, gate, near, far, own, other, after)


def shared_first_kernel(place, feed, own, other, _, part):
    quarter = own.shape[0]
    rows = part.shape[0] // 2
    here = pl.multiple_of(place[0] * quarter, quarter)
    there = pl.multiple_of((1 - place[0]) * quarter, quarter)
    total = dot(feed[0 : 2 * rows, pl.ds(here, quarter)], own[...])
    total += dot(feed[0 : 2 * rows, pl.ds(there, quarter)], other[...])
    for b in range(2):
        turn = place[1] if b == 0 else 1 - place[1]
        at = pl.ds(pl.multiple_of(turn * rows, rows), rows)
        part[at, :] = total[b * rows : (b + 1) * rows].astype(BF16)


def shared_second_kernel(place, near, far, own, other, _, out):
    quarter = own.shape[1]
    rows = near.shape[0] // 2
    here = pl.multiple_of(place[0] * quarter, quarter)
    there = pl.multiple_of((1 - place[0]) * quarter, quarter)
    hidden = jax.nn.gelu(near[...].astype(F32) + far[...].astype(F32)).astype(BF16)
    left, right = dot(hidden, own[...]), dot(hidden, other[...])
    for b in range(2):
        turn = place[1] if b == 0 else 1 - place[1]
        at = pl.ds(pl.multiple_of(turn * rows, rows), rows)
        out[at, pl.ds(here, quarter)] = left[b * rows : (b + 1) * rows]
        out[at, pl.ds(there, quarter)] = right[b * rows : (b + 1) * rows]


def take_stage(place, source, own, after, grant, lead, count):
    shape = (count, *source.shape[1:])
    return pl.pallas_call(
        functools.partial(take_kernel, own, lead),
        in_specs=[SMEM, HBM, ANY],
        out_specs=VMEM,
        out_shape=jax.ShapeDtypeStruct(shape, BF16),
        scratch_shapes=[pltpu.SemaphoreType.DMA(shape[:1])],
        compiler_params=granted(grant),
        cost_estimate=cost(KERNEL_FLOPS, 4 * shape[0] * shape[1] * shape[2]),
    )(place, source, after)


def kernel(body, after, shapes, place, *args):
    return pl.pallas_call(
        body,
        in_specs=[SMEM] + [VMEM] * len(args) + [ANY],
        out_specs=[VMEM] * len(shapes),
        out_shape=shapes,
        compiler_params=granted(),
        cost_estimate=cost(KERNEL_FLOPS, 1 << 20),
    )(place, *args, after)


def exchanged_partials(tokens, expert_ids, gate_weights, expert_in, expert_out, shared_in, shared_out):
    rows, width = tokens.shape
    half = width // 2
    picks = expert_ids.shape[1]
    group = expert_in.shape[0]
    local = group // 2
    hidden = expert_in.shape[2]
    groups = lax.axis_size(GROUP)
    spot = lax.axis_index(SIDE)
    side, core = spot // 2, spot % 2
    lead = lax.axis_index(GROUP) * group + core * local
    place = jnp.stack([core, side, lead]).astype(jnp.int32)

    def swap(value, axis, mask):
        return lax.ppermute(value, axis, [(i, i ^ mask) for i in range(lax.axis_size(axis))])

    def cross(value):
        return swap(value, SIDE, 2)

    def share(value):
        return swap(value, SIDE, 1)

    def take(source, own, after, grant, lead=0, count=local):
        return take_stage(place, source, own, after, grant, lead, count)

    give_in = take(expert_in, False, place, GIVE_GRANTS[0], 0, local // 2)
    other_in = [share(give_in)]
    block = jax.ShapeDtypeStruct((rows + META, half), BF16)
    mine, theirs = kernel(
        norm_kernel, give_in, [block] * 2,
        place, tokens, expert_ids.T, gate_weights.T,
    )
    peer = cross(theirs)
    give_in = take(expert_in, False, mine, GIVE_GRANTS[0], local // 2, local // 2)
    other_in.append(share(give_in))
    own_in = take(expert_in, True, give_in, GIVE_GRANTS[1])
    far = far_groups(groups)
    feeds = {"o": [mine, peer]}
    feeds["n"] = [swap(mine, GROUP, 1), swap(peer, GROUP, 1)]
    for g in far:
        if g % 2:
            early = swap(mine, GROUP, g)
            got = pair_up(early, swap(peer, GROUP, g), rows)
        else:
            got = swap(feeds[str(g + 1)][0], GROUP, 1)
        feeds[str(g)] = [got, share(got)]
    if far:
        feeds["m"] = [feeds["2"].pop()]

    firsts, kept, sums = {}, {}, []
    last, own_out = own_in, None

    def first(g):
        nonlocal last
        part, code, gate, *pair = first_stage(feeds[g], rows, place, own_in, other_in, last, picks)
        firsts[g] = (part, code, gate, cross(part))
        last = code
        return pair

    def second(g):
        nonlocal last, own_out
        part, code, gate, across = firsts[g]
        load = own_out is None
        keep, send, join = g not in "ltm2", g not in "on2", g == "2"
        outs = second_stage(
            code.shape[1] // (2 * rows), code, gate, part, across, place, expert_out if load else own_out,
            other_out, kept["m"] if join else last, keep, send, join, load,
        )
        last = outs[0]
        own_out = outs[-1] if load else own_out
        if keep:
            kept[g] = outs[0]
        if join:
            sums.append(swap(last, GROUP, 2).astype(F32))
        if not send:
            return
        came = share(outs[keep])
        if g == "m":
            kept[g] = came
            return
        came = came.astype(F32)
        if g != "t":
            last = (kept.pop("n" if g == "l" else g) + came).astype(BF16)
            came = swap(last, GROUP, 1 if g == "l" else int(g)).astype(F32)
        sums.append(came)

    (unit,) = first("o")
    feeds["t"] = [share(unit)]
    last = give_out = take(expert_out, False, last, GIVE_GRANTS[2])
    other_out = share(give_out)
    other_shared_in = share(shared_in)
    other_shared_out = share(shared_out)
    tail = [str(g) for g in far[:-1]] + ["m", "2"] * bool(far)
    (near,) = first("n")
    feeds["l"] = [share(near)]
    first("l")
    second("o")
    for g in tail[:1]:
        first(g)
    second("n")
    second("l")
    for g in tail[1:]:
        first(g)
    first("t")
    (shared_part,) = kernel(
        shared_first_kernel, last,
        [jax.ShapeDtypeStruct((2 * rows, hidden), BF16)],
        place, unit, shared_in, other_shared_in,
    )
    last = shared_part
    shared_far = cross(shared_part)
    for g in [*tail, "t"]:
        second(g)
    (shared,) = kernel(
        shared_second_kernel, last,
        [jax.ShapeDtypeStruct((2 * rows, half), F32)],
        place, shared_part, shared_far, shared_out, other_shared_out,
    )

    total = sum(sums, shared + kept["o"])
    crossed = cross(total[rows:].astype(BF16)).astype(F32)
    stay = total[:rows]
    low = side == 0
    added = jnp.concatenate([jnp.where(low, stay, crossed), jnp.where(low, crossed, stay)], axis=1)
    return (tokens.astype(F32) + added).astype(BF16)


def exchange_fits(mesh, tokens, expert_ids, expert_in):
    groups, sides = mesh.shape[GROUP], mesh.shape[SIDE]
    blocks = mesh.shape[SWEEP] * groups
    rows, width = tokens.shape[0] // (blocks * sides), tokens.shape[1]
    return (
        sides == 4
        and expert_in.shape[0] % (blocks * 16) == 0
        and groups in (4, 8)
        and rows % 128 == 0
        and width % 512 == 0
        and width // 2 >= 3 * rows
        and expert_ids.shape[1] <= META
        and expert_in.shape[2] % 128 == 0
    )


def pair_up(first, second, rows):
    return jnp.concatenate([first[:rows], second[:rows], first[rows:], second[rows:]], axis=0)


def far_groups(groups):
    return list(range(groups - 1, 1, -1))


def solution(mesh):
    rows = P((SWEEP, GROUP, SIDE), None)
    placed = (
        rows,
        rows,
        rows,
        P((SWEEP, GROUP), SIDE, None),
        P((SWEEP, GROUP), None, SIDE),
        P((SWEEP, SIDE), None),
        P(SWEEP, SIDE),
    )
    spread = functools.partial(
        jax.shard_map, mesh=mesh, in_specs=placed, out_specs=rows, check_vma=False
    )

    def program(*args):
        if not exchange_fits(mesh, args[0], args[1], args[3]):
            return spread(gathered_weights)(*args)
        step = spread(exchanged_partials)
        return step(*args)

    return program
```
